256 devices in a mesh: shuf: 64 (over y, z, core), rep: 4 (over x).
Axes of the slice: x: 4, y: 4, z: 8, core: 2. Of those that a mesh axis runs over, the one named last changes fastest.
Arguments:
- values: bfloat16 [524288, 1024], P('shuf', 'rep')
- subgroup: int32 [4096], P('shuf'), may hold values from 0 to 31
- owners: int32 [4096, 1], P('shuf'), may hold values from 0 to 63; in each aligned block of 64 rows (0 to 63, 64 to 127, ...) at most 2 rows name the same one
- col_gain: float32 [1024], P('rep'), may hold values from 0.5 to 1.5
- col_bias: float32 [1024], P('rep'), may hold values from -3 to 3
- out_weight: bfloat16 [1024, 1024], P('rep'), may hold values from -0.1875 to 0.1875
Outputs:
- projected: bfloat16 [524288, 1024], P(('shuf', 'rep'))
The draws below stay inside these ranges and needn't reach their ends.
Inputs may be any that keep to these rules, and one draw needn't show every extreme that they name: `owners`: among the tiles of one index of shuf no owner is named more than 2 times, a bound that some block reaches.
All inputs are finite; a program needn't handle non-finite values.
Results may differ from the reference program's by a relative error of at most 0.015.
Values may be sent and summed in bfloat16 or wider, within the bound.
No kernel may reach another device: no remote copies, remote signals or barrier semaphores. Data moves between devices by JAX's collectives and lax.ppermute only.
A program may use at most 64 MiB of HBM per device.

```python
import math
import jax
import jax.numpy as jnp
import numpy as np
from jax import lax

TILE = 128
TILES_DEV = 64
COLS = 1024
OUT = 1024
GRP_DEV = 32
PRIOR = 256
ROWS_DEV = 8192
TILES = 4096
ROWS = 524288
CAP = 2
N_SHUF = 64
N_REP = 4


def draw_values(key, part):
    keys = jax.random.split(jax.random.fold_in(key, 11), 7)
    blocks = ROWS // ROWS_DEV
    place = jnp.arange(ROWS, dtype=jnp.float32).reshape(TILES, TILE, 1) / float(ROWS)
    rough = jax.random.uniform(keys[0], (TILES, TILE, 1), minval=0.7, maxval=1.4)
    row_scale = jnp.exp(jnp.log(3.0) * place) * rough
    shift = 1.5 * jax.random.normal(keys[4], (blocks, 1, COLS))
    shift_rows = jnp.repeat(shift, TILES_DEV, axis=0)
    chosen = jax.random.bernoulli(keys[5], 0.5, (TILES, 1, COLS))
    stretch = jnp.exp(jax.random.uniform(keys[6], (TILES, 1, COLS), minval=-0.6, maxval=0.6))
    factor = jnp.where(chosen, stretch, 1.0)
    col_scale = jnp.exp(jax.random.uniform(keys[1], (1, 1, COLS), minval=0.0, maxval=jnp.log(10.0)))
    noise = jax.random.normal(keys[2], (TILES, TILE, COLS))
    offset = jax.random.normal(keys[3], (1, 1, COLS)) * (0.5 + 2.0 * place)
    drawn = col_scale * (offset + shift_rows + row_scale * noise * factor)
    return drawn.reshape(ROWS, COLS).astype(jnp.bfloat16)


def set_ends(values, stream_key, low, largest):
    spot = [jax.random.randint(jax.random.fold_in(stream_key, axis), (), 0, length) for axis, length in enumerate(values.shape)]
    widest = values.shape.index(max(values.shape))
    beside = spot[:widest] + [(spot[widest] + 1) % values.shape[widest]] + spot[widest + 1:]
    return values.at[tuple(spot)].set(low).at[tuple(beside)].set(largest)


def level_of(own_key, dims, pieces, smallest, high):
    gain, own = 1.0, jax.random.fold_in(own_key, 6)
    for axis_at, parts in pieces:
        heights = jnp.exp(jax.random.uniform(jax.random.fold_in(own, axis_at), (parts,), jnp.float32, smallest / len(pieces), high / len(pieces)))
        gain = gain * jnp.repeat(heights, dims[axis_at] // parts).reshape([-1 if axis == axis_at else 1 for axis in range(len(dims))])
    return gain


def assign_block(key, own, number, rows, amount, top, most, slope):
    sequence = jax.random.permutation(key, amount)
    heavy_load, ordinary = load_shares(amount, rows * top, most, slope, True), load_shares(amount, rows * top, most, slope, False)
    places = jnp.arange(amount)

    def named(tallies, offset_by):
        used = int((tallies > 0).sum())
        fixed = max(1, used // 4)
        passed = fixed + (places - fixed + offset_by * (used - fixed)) % max(1, amount - fixed)
        return jnp.zeros((amount,), jnp.int32).at[sequence[jnp.where(places < fixed, places, passed)]].set(jnp.asarray(tallies, jnp.int32))

    tallies = jnp.where(number % 4 == 0, named(heavy_load, number // 4), named(ordinary, number - number // 4 - 1))
    mixed = jax.random.permutation(jax.random.fold_in(own, 3), amount)
    source_of, sink = mixed[0:amount // 2 * 2:2], mixed[1:amount // 2 * 2:2]
    margin = jnp.minimum(tallies[source_of] - 1, most - tallies[sink]) // 2
    margin = jnp.where((source_of == sequence[0]) | (sink == sequence[0]) | (tallies[sink] == 0), 0, jnp.maximum(margin, 0))
    passed = jax.random.randint(jax.random.fold_in(own, 4), (amount // 2,), 0, 1 << 20) % (margin + 1)
    tallies = tallies.at[source_of].add(-passed).at[sink].add(passed)
    labels = jnp.searchsorted(jnp.cumsum(tallies), jnp.arange(rows * top), side="right").astype(jnp.int32)
    listing = labels.reshape(top, rows).T
    listing = listing[jax.random.permutation(jax.random.fold_in(own, 1), rows)]
    offset_by = jax.random.randint(jax.random.fold_in(own, 2), (rows, 1), 0, top)
    return jnp.take_along_axis(listing, (jnp.arange(top)[None, :] + offset_by) % top, axis=1)


def load_shares(count, total, limit, slope, full):
    portions = [(1 << 20) // math.isqrt(rank ** slope) + 1 for rank in range(1, count + 1)]
    largest = limit if full else min(limit, max(-(-total // count), total * portions[0] // sum(portions)))
    least = 1 if total - largest >= count - 1 else 0
    counts, surplus = [largest] + [least] * (count - 1), total - largest - least * (count - 1)
    while surplus > 0:
        movable = [i for i in range(1, count) if counts[i] < largest] or [i for i in range(1, count) if counts[i] < limit]
        whole, remaining = sum([portions[i] for i in movable]), surplus
        for i in movable:
            more = min(limit - counts[i], max(1, remaining * portions[i] // whole), surplus)
            counts[i] = counts[i] + more
            surplus = surplus - more
    return np.array(counts)


def normal_values(stream_key, extent, scale, reach, shards=(), held_as=jnp.bfloat16):
    result = scale * jax.random.normal(stream_key, extent, jnp.float32)
    if shards:
        result = result * level_of(stream_key, extent, shards, -0.22, 0.18)
    return jnp.clip(result, -reach, reach).astype(held_as)


def setup_inputs(seed: int = 0) -> dict:
    key_list = jax.random.split(jax.random.key(seed), 7)
    values = draw_values(jax.random.fold_in(key_list[6], 71), 0)
    subgroup = set_ends(jax.random.randint(key_list[1], (TILES,), 0, GRP_DEV), jax.random.fold_in(key_list[1], 1), 0, GRP_DEV - 1).astype(jnp.int32)
    owners_keys = jax.random.split(jax.random.fold_in(key_list[2], 1), TILES // TILES_DEV)
    owners_turns = jax.random.permutation(jax.random.fold_in(key_list[2], 3), TILES // TILES_DEV)
    owners = jax.vmap(lambda own, number: assign_block(jax.random.fold_in(key_list[2], 2), own, number, TILES_DEV, N_SHUF, 1, CAP, 1))(owners_keys, owners_turns).reshape((TILES, 1))
    col_gain = jnp.clip(1.0 + 0.1 * jax.random.normal(key_list[3], (COLS,), jnp.float32), 0.5, 1.5)
    col_bias = normal_values(key_list[4], (COLS,), 0.5, 3.0, ((0, 4),), jnp.float32)
    out_weight = normal_values(key_list[5], (COLS, OUT), COLS ** -0.5, 0.1875, ((0, 4),))
    return {"values": values, "subgroup": subgroup, "owners": owners, "col_gain": col_gain, "col_bias": col_bias, "out_weight": out_weight}


def reference(values, subgroup, owners, col_gain, col_bias, out_weight):
    row_total, col_total = values.shape
    tile_total = row_total // TILE
    groups = GRP_DEV * N_SHUF
    group = (owners[:, 0] * GRP_DEV + subgroup).astype(jnp.int32)
    shaped = values.astype(jnp.float32).reshape(tile_total, TILE, col_total)
    tile_sum = lax.optimization_barrier(jnp.sum(shaped, axis=1))
    tile_sq = lax.optimization_barrier(jnp.sum(shaped * shaped, axis=1))
    group_sum = jax.ops.segment_sum(tile_sum, group, num_segments=groups)
    group_sq = jax.ops.segment_sum(tile_sq, group, num_segments=groups)
    count = jax.ops.segment_sum(jnp.full((tile_total,), float(TILE), jnp.float32), group, num_segments=groups)
    mean_all = lax.optimization_barrier(jnp.sum(tile_sum, axis=0)) / float(row_total)
    square_all = lax.optimization_barrier(jnp.sum(tile_sq, axis=0)) / float(row_total)
    weight = (count + float(PRIOR))[:, None]
    center = (group_sum + float(PRIOR) * mean_all) / weight
    second = (group_sq + float(PRIOR) * square_all) / weight
    inverse = lax.rsqrt(second - center * center + 1e-05)
    tile_center = center[group]
    tile_scale = inverse[group] * col_gain
    scored = ((shaped - tile_center[:, None, :]) * tile_scale[:, None, :] + col_bias).astype(jnp.bfloat16)
    scored = scored.reshape(row_total, col_total)
    block_cols = col_total // N_REP
    summed = jnp.zeros((row_total, out_weight.shape[1]), jnp.float32)
    for block in range(N_REP):
        partial_value = jnp.dot(scored[:, block * block_cols:(block + 1) * block_cols], out_weight[block * block_cols:(block + 1) * block_cols], preferred_element_type=jnp.float32)
        summed = summed + partial_value.astype(jnp.bfloat16).astype(jnp.float32)
    return summed.astype(jnp.bfloat16)
```

```python
import jax
import jax.numpy as jnp
from jax import lax
from jax.experimental import pallas as pl
from jax.experimental.pallas import tpu as pltpu
from jax.sharding import PartitionSpec as P

PRIOR = 256.0
LANES = 128
MSG = 16
F32 = jnp.float32
BF16 = jnp.bfloat16
HIGHEST = lax.Precision.HIGHEST


def iota(shape, dim):
    return lax.broadcasted_iota(jnp.int32, shape, dim)


def exact_dot(one_hot, rows):
    return jnp.dot(one_hot.astype(BF16), rows.astype(BF16), preferred_element_type=F32)


def as_column(row, size, at):
    picked = jnp.where(at == iota((size, size), 1), jnp.broadcast_to(row, (size, size)), 0.0)
    return jnp.sum(picked, axis=1, keepdims=True)


def places(owner_row):
    size = owner_row.shape[1]
    column = as_column(owner_row, size, iota((size, size), 0))
    same = column == jnp.broadcast_to(owner_row, (size, size))
    earlier = iota((size, size), 0) < iota((size, size), 1)
    return jnp.sum(jnp.where(same & earlier, 1.0, 0.0), axis=0, keepdims=True)


def put(scratch, part, peers, at):
    for n in range(part.shape[1] // LANES):
        scratch[pl.ds(at + n, peers, stride=MSG), :] = part[:, n * LANES : (n + 1) * LANES]


def take(scratch, peers, at, count):
    return jnp.concatenate([scratch[pl.ds(at + n, peers, stride=MSG), :] for n in range(count)], axis=1)


def stats_kernel(values, owner, sub, out, mean, var, scratch, *, tiles, peers):
    step = pl.program_id(0)
    rows, cols = values.shape
    here = tiles // pl.num_programs(0)
    wide = values[...].astype(F32).reshape(here, rows // here, cols)
    inverse_rows = 1.0 / (rows // here)
    tile_mean = jnp.sum(wide, axis=1) * inverse_rows
    tile_var = jnp.sum(wide * wide, axis=1) * inverse_rows - tile_mean * tile_mean
    at = pl.multiple_of(step * here, here)
    mean[pl.ds(at, here), :] = tile_mean
    var[pl.ds(at, here), :] = tile_var

    @pl.when(step == pl.num_programs(0) - 1)
    def _():
        all_mean, all_var = mean[...], var[...]
        dev_mean = jnp.sum(all_mean, axis=0, keepdims=True) * (1.0 / tiles)
        apart = all_mean - dev_mean
        dev_var = jnp.sum(all_var + apart * apart, axis=0, keepdims=True) * (1.0 / tiles)
        owner_row = owner[...].astype(F32)
        place = places(owner_row)
        named = jnp.broadcast_to(owner_row, (peers, tiles)) == iota((peers, tiles), 0).astype(F32)
        sub_column = as_column(sub[...].astype(F32), tiles, iota((tiles, tiles), 0))
        sub_wide = jnp.broadcast_to(sub_column + 1.0, (tiles, LANES))
        for slot in range(2):
            hot = jnp.where(named & (place == float(slot)), 1.0, 0.0)
            put(scratch, exact_dot(hot, all_mean), peers, 4 * slot)
            put(scratch, exact_dot(hot, all_var), peers, 4 * slot + 2)
            put(scratch, exact_dot(hot, sub_wide) - 1.0, peers, 14 + slot)
        high = dev_mean.astype(BF16).astype(F32)
        put(scratch, jnp.broadcast_to(high, (peers, cols)), peers, 8)
        put(scratch, jnp.broadcast_to(dev_mean - high, (peers, cols)), peers, 10)
        put(scratch, jnp.broadcast_to(dev_var, (peers, cols)), peers, 12)
        out[...] = scratch[...].astype(BF16)


def owner_kernel(arrived, gain, bias, out, scratch, *, peers, tile_rows):
    scratch[...] = arrived[...].astype(F32)
    dev_mean = take(scratch, peers, 8, 2) + take(scratch, peers, 10, 2)
    mean_all = jnp.sum(dev_mean, axis=0, keepdims=True) * (1.0 / peers)
    apart = dev_mean - mean_all
    var_all = jnp.sum(take(scratch, peers, 12, 2) + apart * apart, axis=0, keepdims=True) * (1.0 / peers)
    hots, firsts, seconds = [], [], []
    for slot in range(2):
        label = take(scratch, peers, 14 + slot, 1)
        hots.append(jnp.where(label == iota((peers, LANES), 1).astype(F32), 1.0, 0.0))
        shifted = take(scratch, peers, 4 * slot, 2) - mean_all
        firsts.append(shifted)
        seconds.append(take(scratch, peers, 4 * slot + 2, 2) + shifted * shifted)
    hot = jnp.concatenate(hots, axis=0)
    data = jnp.concatenate([jnp.concatenate(firsts, axis=0), jnp.concatenate(seconds, axis=0)], axis=1)

    def by_group(rows):
        return lax.dot_general(hot, rows, (((0,), (0,)), ((), ())), precision=HIGHEST, preferred_element_type=F32)

    cols = dev_mean.shape[1]
    sums = by_group(data) * float(tile_rows)
    count = by_group(jnp.ones((2 * peers, LANES), F32)) * float(tile_rows)
    weight = jnp.concatenate([count + PRIOR] * (cols // LANES), axis=1)
    center = sums[:, :cols] / weight
    second = (sums[:, cols:] + PRIOR * var_all) / weight
    inverse = lax.rsqrt(second - center * center + 1e-05)
    scale = (inverse * gain[...]).astype(BF16)
    shift = bias[...] - (center + mean_all) * scale.astype(F32)
    shift_high = shift.astype(BF16)
    shift_low = (shift - shift_high.astype(F32)).astype(BF16)
    for slot in range(2):
        put(scratch, exact_dot(hots[slot], scale), peers, 6 * slot)
        put(scratch, exact_dot(hots[slot], shift_high), peers, 6 * slot + 2)
        put(scratch, exact_dot(hots[slot], shift_low), peers, 6 * slot + 4)
    out[...] = scratch[...].astype(BF16)


def tile_kernel(first, arrived, owner, *refs, tiles, peers, blocks):
    outs, scratch = refs[:-1], refs[-1]
    scratch[...] = arrived[...].astype(F32)
    owner_row = owner[...].astype(F32)
    at = (iota((tiles, tiles), 0) + first[0]) % tiles
    place = as_column(places(owner_row), tiles, at)
    named = as_column(owner_row, tiles, at) == iota((tiles, peers), 1).astype(F32)
    picked = 0.0
    for slot in range(2):
        hot = jnp.where(named & (place == float(slot)), 1.0, 0.0)
        picked = picked + exact_dot(hot, take(scratch, peers, 6 * slot, 6))
    each = tiles // blocks
    for n, out in enumerate(outs):
        out[...] = picked[n * each : (n + 1) * each, :].astype(BF16)


def project_kernel(*refs, blocks, tile_rows):
    values, coeffs, weights = refs[:blocks], refs[blocks : 2 * blocks], refs[2 * blocks : 3 * blocks]
    out, wide = refs[3 * blocks :]
    step = pl.program_id(0)
    rows, cols = values[0].shape

    @pl.when(step == 0)
    def _():
        for n in range(blocks):
            wide[n] = coeffs[n][...].astype(F32)

    tiles = rows // tile_rows
    total = None
    for n in range(blocks):
        parts = []
        for t in range(tiles):
            row = wide[n, pl.ds(step * tiles + t, 1), :]
            value = values[n][t * tile_rows : (t + 1) * tile_rows, :].astype(F32)
            scored = value * row[:, :cols] + (row[:, cols : 2 * cols] + row[:, 2 * cols :])
            parts.append(scored.astype(BF16))
        part = jnp.dot(jnp.concatenate(parts, axis=0), weights[n][...], preferred_element_type=F32)
        total = part if total is None else total + part
    out[...] = total.astype(BF16)


def hop(value, axis, distance):
    size = lax.axis_size(axis)
    return lax.ppermute(value, axis, [(i, (i + distance) % size) for i in range(size)])


def whole(*shape):
    return pl.BlockSpec(shape, lambda *_: (0,) * len(shape))


def on_device(values, subgroup, owners, col_gain, col_bias, out_weight):
    rows, cols = values.shape
    tiles = subgroup.shape[0]
    tile_rows = rows // tiles
    peers, blocks = lax.axis_size("shuf"), lax.axis_size("rep")
    rank = lax.axis_index("rep")
    own_rows = rows // blocks
    outputs = out_weight.shape[1]
    owner_row, sub_row = owners.reshape(1, tiles), subgroup.reshape(1, tiles)

    pieces = [
        lax.dynamic_slice(values, (((rank + d) % blocks) * own_rows, 0), (own_rows, cols))
        for d in range(blocks)
    ]
    mine, sent = pieces[0], pieces[1:]
    moved = [mine]
    for d in range(1, blocks):
        moved.append(hop(sent[d - 1], "rep", d))
    weights = [out_weight]
    for d in range(1, blocks):
        weights.append(hop(out_weight, "rep", d))

    steps = 8
    outgoing = pl.pallas_call(
        lambda *refs: stats_kernel(*refs, tiles=tiles, peers=peers),
        grid=(steps,),
        in_specs=[
            pl.BlockSpec((rows // steps, cols), lambda i: (i, 0)),
            whole(1, tiles),
            whole(1, tiles),
        ],
        out_specs=whole(peers * MSG, LANES),
        out_shape=jax.ShapeDtypeStruct((peers * MSG, LANES), BF16),
        scratch_shapes=[
            pltpu.VMEM((tiles, cols), F32),
            pltpu.VMEM((tiles, cols), F32),
            pltpu.VMEM((peers * MSG, LANES), F32),
        ],
        name="stats",
    )(values, owner_row, sub_row)

    def exchange(message):
        arrived = lax.all_to_all(message.reshape(peers, MSG, LANES), "shuf", 0, 0, tiled=True)
        return arrived.reshape(peers * MSG, LANES)

    arrived = exchange(outgoing)
    answer = pl.pallas_call(
        lambda *refs: owner_kernel(*refs, peers=peers, tile_rows=tile_rows),
        out_shape=jax.ShapeDtypeStruct((peers * MSG, LANES), BF16),
        scratch_shapes=[pltpu.VMEM((peers * MSG, LANES), F32)],
        name="moments",
    )(arrived, col_gain.reshape(1, cols), col_bias.reshape(1, cols))
    returned = exchange(answer)
    each = tiles // blocks
    coeffs = pl.pallas_call(
        lambda *refs: tile_kernel(*refs, tiles=tiles, peers=peers, blocks=blocks),
        in_specs=[
            pl.BlockSpec(memory_space=pltpu.SMEM),
            whole(peers * MSG, LANES),
            whole(1, tiles),
        ],
        out_specs=[whole(each, 3 * cols)] * blocks,
        out_shape=[jax.ShapeDtypeStruct((each, 3 * cols), BF16)] * blocks,
        scratch_shapes=[pltpu.VMEM((peers * MSG, LANES), F32)],
        name="pick",
    )((rank * each).reshape(1), returned, owner_row)
    known = [coeffs[0]]
    for d in range(1, blocks):
        known.append(hop(coeffs[d], "rep", d))

    block = min(512, own_rows)
    return pl.pallas_call(
        lambda *refs: project_kernel(*refs, blocks=blocks, tile_rows=tile_rows),
        grid=(own_rows // block,),
        in_specs=[pl.BlockSpec((block, cols), lambda i: (i, 0))] * blocks
        + [whole(each, 3 * cols)] * blocks
        + [whole(cols, outputs)] * blocks,
        out_specs=pl.BlockSpec((block, outputs), lambda i: (i, 0)),
        out_shape=jax.ShapeDtypeStruct((own_rows, outputs), BF16),
        scratch_shapes=[pltpu.VMEM((blocks, each, 3 * cols), F32)],
        name="project",
    )(*moved, *known, *weights)


def solution(mesh):
    return jax.shard_map(
        on_device,
        mesh=mesh,
        in_specs=(P("shuf", "rep"), P("shuf"), P("shuf", None), P("rep"), P("rep"), P("rep", None)),
        out_specs=P(("shuf", "rep"), None),
        check_vma=False,
    )
```

```python
import jax
import jax.numpy as jnp
from jax import lax
from jax.experimental import pallas as pl
from jax.experimental.pallas import tpu as pltpu
from jax.sharding import PartitionSpec as P

GRP_DEV = 32
PRIOR = 256.0
LANES = 128
MSG = 16
F32 = jnp.float32
BF16 = jnp.bfloat16
MIB = 1 << 20


def iota(shape, dim):
    return lax.broadcasted_iota(jnp.int32, shape, dim)


def exact_dot(one_hot, rows):
    return jnp.dot(one_hot.astype(BF16), rows.astype(BF16), preferred_element_type=F32)


def as_column(row, size, at):
    picked = jnp.where(at == iota((size, size), 1), jnp.broadcast_to(row, (size, size)), 0.0)
    return jnp.sum(picked, axis=1, keepdims=True)


def places(owner_row):
    size = owner_row.shape[1]
    column = as_column(owner_row, size, iota((size, size), 0))
    same = column == jnp.broadcast_to(owner_row, (size, size))
    earlier = iota((size, size), 0) < iota((size, size), 1)
    return jnp.sum(jnp.where(same & earlier, 1.0, 0.0), axis=0, keepdims=True)


def put(scratch, part, peers, at):
    for n in range(part.shape[1] // LANES):
        scratch[pl.ds(at + n, peers, stride=MSG), :] = part[:, n * LANES : (n + 1) * LANES]


def take(scratch, peers, at, count):
    return jnp.concatenate([scratch[pl.ds(at + n, peers, stride=MSG), :] for n in range(count)], axis=1)


def cut_kernel(start, *refs, count, rows):
    sources, outs, sems = refs[:count], refs[count : 2 * count], refs[2 * count]
    copies = [
        pltpu.make_async_copy(sources[n].at[pl.ds(pl.multiple_of(start[n], rows[n]), rows[n]), :], outs[n], sems.at[n])
        for n in range(count)
    ]
    for copy in copies:
        copy.start()
    for copy in copies:
        copy.wait()


def stack_kernel(*refs):
    parts, out = refs[:-1], refs[-1]
    rows = parts[0].shape[0]
    for n, part in enumerate(parts):
        out[n * rows : (n + 1) * rows, :] = part[...]


def stats_kernel(values, owner, sub, out, first, second, scratch, *, tiles, peers):
    step = pl.program_id(0)
    rows, cols = values.shape
    here = tiles // pl.num_programs(0)
    tile_rows = rows // here
    chunk = 16

    def one_tile(t, carry):
        low = high = None
        for n in range(tile_rows // chunk):
            at = pl.multiple_of(t * tile_rows + n * chunk, chunk)
            wide = values[pl.ds(at, chunk), :].astype(F32)
            low, high = (wide, wide * wide) if low is None else (low + wide, high + wide * wide)
        at = pl.multiple_of((step * here + t) * 8, 8)
        for n in range(cols // LANES):
            lanes = slice(n * LANES, (n + 1) * LANES)
            first[n, pl.ds(at, 8), :] = low[:8, lanes] + low[8:, lanes]
            second[n, pl.ds(at, 8), :] = high[:8, lanes] + high[8:, lanes]
        return carry

    lax.fori_loop(0, here, one_tile, 0, unroll=2)

    @pl.when(step == pl.num_programs(0) - 1)
    def _():
        def folded(ref):
            halves = []
            for n in range(cols // LANES):
                rows = [ref[n, pl.ds(r, tiles, stride=8), :] for r in range(8)]
                while len(rows) > 1:
                    rows = [a + b for a, b in zip(rows[::2], rows[1::2])]
                halves.append(rows[0])
            return jnp.concatenate(halves, axis=1) * (1.0 / tile_rows)

        all_mean = folded(first)
        all_var = folded(second) - all_mean * all_mean
        dev_mean = jnp.sum(all_mean, axis=0, keepdims=True) * (1.0 / tiles)
        apart = all_mean - dev_mean
        dev_var = jnp.sum(all_var + apart * apart, axis=0, keepdims=True) * (1.0 / tiles)
        owner_row = owner[...].astype(F32)
        place = places(owner_row)
        named = jnp.broadcast_to(owner_row, (peers, tiles)) == iota((peers, tiles), 0).astype(F32)
        sub_column = as_column(sub[...].astype(F32), tiles, iota((tiles, tiles), 0))
        sub_wide = jnp.broadcast_to(sub_column + 1.0, (tiles, LANES))
        hot = jnp.concatenate([jnp.where(named & (place == float(slot)), 1.0, 0.0) for slot in range(2)], axis=0)
        sent = exact_dot(hot, jnp.concatenate([all_mean, all_var, sub_wide], axis=1))
        for slot in range(2):
            here = sent[slot * peers : (slot + 1) * peers, :]
            put(scratch, here[:, : 2 * cols], peers, 4 * slot)
            put(scratch, here[:, 2 * cols :] - 1.0, peers, 14 + slot)
        high = dev_mean.astype(BF16).astype(F32)
        put(scratch, jnp.broadcast_to(high, (peers, cols)), peers, 8)
        put(scratch, jnp.broadcast_to(dev_mean - high, (peers, cols)), peers, 10)
        put(scratch, jnp.broadcast_to(dev_var, (peers, cols)), peers, 12)
        out[...] = scratch[...].astype(BF16)


def owner_kernel(arrived, gain, bias, out, scratch, *, peers, tile_rows):
    scratch[...] = arrived[...].astype(F32)
    dev_mean = take(scratch, peers, 8, 2) + take(scratch, peers, 10, 2)
    mean_all = jnp.sum(dev_mean, axis=0, keepdims=True) * (1.0 / peers)
    apart = dev_mean - mean_all
    var_all = jnp.sum(take(scratch, peers, 12, 2) + apart * apart, axis=0, keepdims=True) * (1.0 / peers)
    cols = dev_mean.shape[1]
    forth, back, firsts, seconds = [], [], [], []
    for slot in range(2):
        label = take(scratch, peers, 14 + slot, 1)
        back.append(jnp.where(label[:, :GRP_DEV] == iota((peers, GRP_DEV), 1).astype(F32), 1.0, 0.0))
        on_diagonal = iota((peers, peers), 0) == iota((peers, peers), 1)
        row = jnp.sum(jnp.where(on_diagonal, label[:, :peers], 0.0), axis=0, keepdims=True)
        wide = jnp.broadcast_to(row, (GRP_DEV, peers))
        forth.append(jnp.where(wide == iota((GRP_DEV, peers), 0).astype(F32), 1.0, 0.0))
        shifted = take(scratch, peers, 4 * slot, 2) - mean_all
        firsts.append(shifted)
        seconds.append(take(scratch, peers, 4 * slot + 2, 2) + shifted * shifted)
    forth = jnp.concatenate(forth, axis=1)
    count = jnp.sum(forth, axis=1, keepdims=True) * float(tile_rows)
    data = jnp.concatenate([jnp.concatenate(firsts, axis=0), jnp.concatenate(seconds, axis=0)], axis=1)
    high = data.astype(BF16).astype(F32)
    middle = (data - high).astype(BF16).astype(F32)
    parts = exact_dot(forth, jnp.concatenate([high, middle, data - high - middle], axis=1))
    sums = (parts[:, : 2 * cols] + parts[:, 2 * cols : 4 * cols] + parts[:, 4 * cols :]) * float(tile_rows)
    portion = 1.0 / (count + PRIOR)
    center = sums[:, :cols] * portion
    second = (sums[:, cols:] + PRIOR * var_all) * portion
    inverse = lax.rsqrt(second - center * center + 1e-05)
    scale = (inverse * gain[...]).astype(BF16).astype(F32)
    shift = bias[...] - (center + mean_all) * scale
    shift_high = shift.astype(BF16).astype(F32)
    reply = exact_dot(
        jnp.concatenate(back, axis=0), jnp.concatenate([scale, shift_high, shift - shift_high], axis=1)
    )
    for slot in range(2):
        put(scratch, reply[slot * peers : (slot + 1) * peers, :], peers, 6 * slot)
    out[...] = scratch[...].astype(BF16)


def tile_kernel(first, arrived, owner, *refs, tiles, peers, blocks):
    outs, scratch = refs[:-1], refs[-1]
    scratch[...] = arrived[...].astype(F32)
    owner_row = owner[...].astype(F32)
    at = (iota((tiles, tiles), 0) + first[0]) % tiles
    place = as_column(places(owner_row), tiles, at)
    named = as_column(owner_row, tiles, at) == iota((tiles, peers), 1).astype(F32)
    hot = jnp.concatenate([jnp.where(named & (place == float(slot)), 1.0, 0.0) for slot in range(2)], axis=1)
    rows = jnp.concatenate([take(scratch, peers, 6 * slot, 6) for slot in range(2)], axis=0)
    picked = exact_dot(hot, rows)
    each = tiles // blocks
    for n, out in enumerate(outs):
        out[...] = picked[n * each : (n + 1) * each, :].astype(BF16)


def project_kernel(place, own, *refs, blocks, tile_rows, slabs):
    moved, coeffs = refs[: blocks - 1], refs[blocks - 1 : 2 * blocks - 1]
    near, far, out, wide, weight = refs[2 * blocks - 1 :]
    step = pl.program_id(0)
    rows, cols = own.shape
    tiles = rows // tile_rows
    slab = near.shape[0] // (slabs * blocks)

    @pl.when(step == 0)
    def _():
        for n in range(blocks):
            wide[n] = coeffs[n][...].astype(F32)
        for e in range(slabs):
            first = lax.rem(place[1] + slabs - e, slabs) * 2
            for n in range(blocks):
                for source, core in ((near, place[2]), (far, 1 - place[2])):
                    at = pl.multiple_of(n * cols + (first + core) * slab, slab)
                    weight[pl.ds(at, slab), :] = source[pl.ds((e * blocks + n) * slab, slab), :]

    strips = []
    for t in range(tiles):
        parts = []
        for n in range(blocks):
            row = wide[n, pl.ds(step * tiles + t, 1), :]
            if n == 0:
                value = own[t * tile_rows : (t + 1) * tile_rows, :]
            else:
                at = pl.multiple_of(step * rows + t * tile_rows, tile_rows)
                value = moved[n - 1][pl.ds(at, tile_rows), :]
            scored = value.astype(F32) * row[:, :cols] + (row[:, cols : 2 * cols] + row[:, 2 * cols :])
            parts.append(scored.astype(BF16))
        strips.append(jnp.concatenate(parts, axis=1))
    out[...] = jnp.dot(jnp.concatenate(strips, axis=0), weight[...], preferred_element_type=F32).astype(BF16)


def hop(value, axis, distance):
    size = lax.axis_size(axis)
    return lax.ppermute(value, axis, [(i, (i + distance) % size) for i in range(size)])


def whole(*shape):
    return pl.BlockSpec(shape, lambda *_: (0,) * len(shape))


IN_VMEM = pl.BlockSpec(memory_space=pltpu.VMEM)
IN_SMEM = pl.BlockSpec(memory_space=pltpu.SMEM)
IN_HBM = pl.BlockSpec(memory_space=pltpu.HBM)


def on_chip(shape, dtype):
    return pltpu.VMEM(shape, dtype)


def limit(mib):
    return pltpu.CompilerParams(vmem_limit_bytes=mib * MIB)


def held(value):
    return pltpu.with_memory_space_constraint(value, pltpu.VMEM)


def off_chip(value):
    return pltpu.with_memory_space_constraint(value, pltpu.HBM)


def cut(start, sources, rows):
    return pl.pallas_call(
        lambda *refs: cut_kernel(*refs, count=len(sources), rows=rows),
        in_specs=[IN_SMEM] + [IN_HBM] * len(sources),
        out_specs=[IN_VMEM] * len(sources),
        out_shape=[on_chip((r, s.shape[1]), s.dtype) for r, s in zip(rows, sources)],
        scratch_shapes=[pltpu.SemaphoreType.DMA((len(sources),))],
        compiler_params=limit(6),
    )(start, *[off_chip(source) for source in sources])


def stacked(parts):
    rows, cols = parts[0].shape
    return pl.pallas_call(
        stack_kernel,
        in_specs=[IN_VMEM] * len(parts),
        out_specs=IN_VMEM,
        out_shape=on_chip((len(parts) * rows, cols), parts[0].dtype),
        compiler_params=limit(6),
    )(*[held(part) for part in parts])


def on_device(values, subgroup, owners, col_gain, col_bias, out_weight):
    rows, cols = values.shape
    tiles = subgroup.shape[0]
    tile_rows = rows // tiles
    peers, blocks = lax.axis_size("shuf"), lax.axis_size("rep")
    rank, index = lax.axis_index("rep"), lax.axis_index("shuf")
    own_rows = rows // blocks
    outputs = out_weight.shape[1]
    owner_row, sub_row = owners.reshape(1, tiles), subgroup.reshape(1, tiles)

    slabs = 4
    depth = peers // (2 * slabs)
    slab_at, core = index // (2 * depth), index % 2
    slab = cols // (2 * slabs)

    def along_slabs(value, e):
        pairs = [(i, (i + e * 2 * depth) % peers) for i in range(peers)]
        return lax.ppermute(value, "shuf", pairs)

    def quarter(d):
        return ((rank + d) % blocks) * own_rows

    moved = {}
    (sent,) = cut(quarter(2).reshape(1), [values], [own_rows])
    moved[2] = hop(sent, "rep", 2)

    steps = 4
    outgoing = pl.pallas_call(
        lambda *refs: stats_kernel(*refs, tiles=tiles, peers=peers),
        grid=(steps,),
        in_specs=[
            pl.BlockSpec((rows // steps, cols), lambda i: (i, 0)),
            whole(1, tiles),
            whole(1, tiles),
        ],
        out_specs=whole(peers * MSG, LANES),
        out_shape=jax.ShapeDtypeStruct((peers * MSG, LANES), BF16),
        scratch_shapes=[
            pltpu.VMEM((cols // LANES, tiles * 8, LANES), F32),
            pltpu.VMEM((cols // LANES, tiles * 8, LANES), F32),
            pltpu.VMEM((peers * MSG, LANES), F32),
        ],
        compiler_params=limit(8),
        name="stats",
    )(off_chip(values), owner_row, sub_row)

    def exchange(message):
        arrived = lax.all_to_all(message.reshape(peers, MSG, LANES), "shuf", 0, 0, tiled=True)
        return held(arrived.reshape(peers * MSG, LANES))

    arrived = exchange(outgoing)

    start = jnp.stack([(slab_at * 2 + core) * slab, quarter(1), quarter(3)])
    own_slab, one, three = cut(start, [out_weight, values, values], [slab, own_rows, own_rows])
    slab_parts = [own_slab]
    for d in range(1, blocks):
        slab_parts.append(hop(own_slab, "rep", d))
    moved[1] = hop(one, "rep", 1)
    moved[3] = hop(three, "rep", 3)

    answer = pl.pallas_call(
        lambda *refs: owner_kernel(*refs, peers=peers, tile_rows=tile_rows),
        in_specs=[IN_VMEM, whole(1, cols), whole(1, cols)],
        out_shape=jax.ShapeDtypeStruct((peers * MSG, LANES), BF16),
        scratch_shapes=[pltpu.VMEM((peers * MSG, LANES), F32)],
        compiler_params=limit(6),
        name="moments",
    )(arrived, col_gain.reshape(1, cols), col_bias.reshape(1, cols))
    returned = exchange(answer)

    one_slab = stacked(slab_parts)
    across = [one_slab]
    for e in range(1, slabs):
        across.append(along_slabs(one_slab, e))
    near = stacked(across)
    far = lax.ppermute(near, "shuf", [(i, i ^ 1) for i in range(peers)])

    each = tiles // blocks
    coeffs = pl.pallas_call(
        lambda *refs: tile_kernel(*refs, tiles=tiles, peers=peers, blocks=blocks),
        in_specs=[IN_SMEM, IN_VMEM, whole(1, tiles)],
        out_specs=[IN_VMEM] * blocks,
        out_shape=[on_chip((each, 3 * cols), BF16)] * blocks,
        scratch_shapes=[pltpu.VMEM((peers * MSG, LANES), F32)],
        compiler_params=limit(4),
        name="pick",
    )((rank * each).reshape(1), returned, owner_row)
    known = {0: coeffs[0]}
    for d in (2, 1, 3):
        known[d] = hop(coeffs[d], "rep", d)

    block = min(512, own_rows)
    inner = [held(moved[d]) for d in range(1, blocks)] + [held(known[d]) for d in range(blocks)]
    inner += [held(near), held(far)]
    return pl.pallas_call(
        lambda *refs: project_kernel(*refs, blocks=blocks, tile_rows=tile_rows, slabs=slabs),
        grid_spec=pltpu.PrefetchScalarGridSpec(
            num_scalar_prefetch=1,
            grid=(own_rows // block,),
            in_specs=[pl.BlockSpec((block, cols), lambda i, place: (place[0] * (own_rows // block) + i, 0))]
            + [IN_VMEM] * len(inner),
            out_specs=pl.BlockSpec((block, outputs), lambda i, place: (i, 0)),
            scratch_shapes=[
                pltpu.VMEM((blocks, each, 3 * cols), F32),
                pltpu.VMEM((blocks * cols, outputs), BF16),
            ],
        ),
        out_shape=jax.ShapeDtypeStruct((own_rows, outputs), BF16),
        compiler_params=limit(24),
        name="project",
    )(jnp.stack([rank, slab_at, core]), off_chip(values), *inner)


def solution(mesh):
    return jax.shard_map(
        on_device,
        mesh=mesh,
        in_specs=(P("shuf", "rep"), P("shuf"), P("shuf", None), P("rep"), P("rep"), P("rep", None)),
        out_specs=P(("shuf", "rep"), None),
        check_vma=False,
    )
```

```python
import jax
import jax.numpy as jnp
from jax import lax
from jax.experimental import pallas as pl
from jax.experimental.pallas import tpu as pltpu
from jax.sharding import PartitionSpec as P

GRP_DEV = 32
PRIOR = 256.0
LANES = 128
MSG = 16
F32 = jnp.float32
BF16 = jnp.bfloat16
MIB = 1 << 20


def iota(shape, dim):
    return lax.broadcasted_iota(jnp.int32, shape, dim)


def exact_dot(one_hot, rows):
    return jnp.dot(one_hot.astype(BF16), rows.astype(BF16), preferred_element_type=F32)


def as_column(row, size, at):
    picked = jnp.where(at == iota((size, size), 1), jnp.broadcast_to(row, (size, size)), 0.0)
    return jnp.sum(picked, axis=1, keepdims=True)


def places(owner_row):
    size = owner_row.shape[1]
    column = as_column(owner_row, size, iota((size, size), 0))
    same = column == jnp.broadcast_to(owner_row, (size, size))
    earlier = iota((size, size), 0) < iota((size, size), 1)
    return jnp.sum(jnp.where(same & earlier, 1.0, 0.0), axis=0, keepdims=True)


def put(scratch, part, peers, at):
    for n in range(part.shape[1] // LANES):
        scratch[pl.ds(at + n, peers, stride=MSG), :] = part[:, n * LANES : (n + 1) * LANES]


def take(scratch, peers, at, count):
    return jnp.concatenate([scratch[pl.ds(at + n, peers, stride=MSG), :] for n in range(count)], axis=1)


def cut_kernel(start, *refs, count, rows):
    sources, outs, sems = refs[:count], refs[count : 2 * count], refs[2 * count]
    copies = [
        pltpu.make_async_copy(sources[n].at[pl.ds(pl.multiple_of(start[n], rows[n]), rows[n]), :], outs[n], sems.at[n])
        for n in range(count)
    ]
    for copy in copies:
        copy.start()
    for copy in copies:
        copy.wait()


def stack_kernel(*refs):
    parts, out, sems = refs[:-2], refs[-2], refs[-1]
    rows = parts[0].shape[0]
    copies = [
        pltpu.make_async_copy(part, out.at[n * rows : (n + 1) * rows, :], sems.at[n]) for n, part in enumerate(parts)
    ]
    for copy in copies:
        copy.start()
    for copy in copies:
        copy.wait()


def stats_kernel(values, owner, sub, out, first, second, scratch, *, tiles, peers):
    step = pl.program_id(0)
    rows, cols = values.shape
    here = tiles // pl.num_programs(0)
    tile_rows = rows // here
    chunk = 16

    def one_tile(t, carry):
        low = high = None
        for n in range(tile_rows // chunk):
            at = pl.multiple_of(t * tile_rows + n * chunk, chunk)
            wide = values[pl.ds(at, chunk), :].astype(F32)
            low, high = (wide, wide * wide) if low is None else (low + wide, high + wide * wide)
        at = pl.multiple_of((step * here + t) * 8, 8)
        for n in range(cols // LANES):
            lanes = slice(n * LANES, (n + 1) * LANES)
            first[n, pl.ds(at, 8), :] = low[:8, lanes] + low[8:, lanes]
            second[n, pl.ds(at, 8), :] = high[:8, lanes] + high[8:, lanes]
        return carry

    lax.fori_loop(0, here, one_tile, 0, unroll=2)

    @pl.when(step == pl.num_programs(0) - 1)
    def _():
        def folded(ref):
            halves = []
            for n in range(cols // LANES):
                rows = [ref[n, pl.ds(r, tiles, stride=8), :] for r in range(8)]
                while len(rows) > 1:
                    rows = [a + b for a, b in zip(rows[::2], rows[1::2])]
                halves.append(rows[0])
            return jnp.concatenate(halves, axis=1) * (1.0 / tile_rows)

        all_mean = folded(first)
        all_var = folded(second) - all_mean * all_mean
        dev_mean = jnp.sum(all_mean, axis=0, keepdims=True) * (1.0 / tiles)
        apart = all_mean - dev_mean
        dev_var = jnp.sum(all_var + apart * apart, axis=0, keepdims=True) * (1.0 / tiles)
        owner_row = owner[...].astype(F32)
        place = places(owner_row)
        named = jnp.broadcast_to(owner_row, (peers, tiles)) == iota((peers, tiles), 0).astype(F32)
        sub_column = as_column(sub[...].astype(F32), tiles, iota((tiles, tiles), 0))
        sub_wide = jnp.broadcast_to(sub_column + 1.0, (tiles, LANES))
        hot = jnp.concatenate([jnp.where(named & (place == float(slot)), 1.0, 0.0) for slot in range(2)], axis=0)
        sent = exact_dot(hot, jnp.concatenate([all_mean, all_var, sub_wide], axis=1))
        for slot in range(2):
            here = sent[slot * peers : (slot + 1) * peers, :]
            put(scratch, here[:, : 2 * cols], peers, 4 * slot)
            put(scratch, here[:, 2 * cols :] - 1.0, peers, 14 + slot)
        high = dev_mean.astype(BF16).astype(F32)
        put(scratch, jnp.broadcast_to(high, (peers, cols)), peers, 8)
        put(scratch, jnp.broadcast_to(dev_mean - high, (peers, cols)), peers, 10)
        put(scratch, jnp.broadcast_to(dev_var, (peers, cols)), peers, 12)
        out[...] = scratch[...].astype(BF16)


def pair_kernel(gain, bias, out):
    out[0:1, :] = gain[...]
    out[1:2, :] = bias[...]


def owner_kernel(arrived, both, out, scratch, *, peers, tile_rows):
    scratch[...] = arrived[...].astype(F32)
    dev_mean = take(scratch, peers, 8, 2) + take(scratch, peers, 10, 2)
    mean_all = jnp.sum(dev_mean, axis=0, keepdims=True) * (1.0 / peers)
    apart = dev_mean - mean_all
    var_all = jnp.sum(take(scratch, peers, 12, 2) + apart * apart, axis=0, keepdims=True) * (1.0 / peers)
    cols = dev_mean.shape[1]
    forth, back, firsts, seconds = [], [], [], []
    for slot in range(2):
        label = take(scratch, peers, 14 + slot, 1)
        back.append(jnp.where(label[:, :GRP_DEV] == iota((peers, GRP_DEV), 1).astype(F32), 1.0, 0.0))
        on_diagonal = iota((peers, peers), 0) == iota((peers, peers), 1)
        row = jnp.sum(jnp.where(on_diagonal, label[:, :peers], 0.0), axis=0, keepdims=True)
        wide = jnp.broadcast_to(row, (GRP_DEV, peers))
        forth.append(jnp.where(wide == iota((GRP_DEV, peers), 0).astype(F32), 1.0, 0.0))
        shifted = take(scratch, peers, 4 * slot, 2) - mean_all
        firsts.append(shifted)
        seconds.append(take(scratch, peers, 4 * slot + 2, 2) + shifted * shifted)
    forth = jnp.concatenate(forth, axis=1)
    count = jnp.sum(forth, axis=1, keepdims=True) * float(tile_rows)
    data = jnp.concatenate([jnp.concatenate(firsts, axis=0), jnp.concatenate(seconds, axis=0)], axis=1)
    high = data.astype(BF16).astype(F32)
    middle = (data - high).astype(BF16).astype(F32)
    parts = exact_dot(forth, jnp.concatenate([high, middle, data - high - middle], axis=1))
    sums = (parts[:, : 2 * cols] + parts[:, 2 * cols : 4 * cols] + parts[:, 4 * cols :]) * float(tile_rows)
    portion = 1.0 / (count + PRIOR)
    center = sums[:, :cols] * portion
    second = (sums[:, cols:] + PRIOR * var_all) * portion
    inverse = lax.rsqrt(second - center * center + 1e-05)
    scale = (inverse * both[0:1, :]).astype(BF16).astype(F32)
    shift = both[1:2, :] - (center + mean_all) * scale
    shift_high = shift.astype(BF16).astype(F32)
    reply = exact_dot(
        jnp.concatenate(back, axis=0), jnp.concatenate([scale, shift_high, shift - shift_high], axis=1)
    )
    for slot in range(2):
        put(scratch, reply[slot * peers : (slot + 1) * peers, :], peers, 6 * slot)
    out[...] = scratch[...].astype(BF16)


def tile_kernel(first, arrived, owner, *refs, tiles, peers, blocks):
    outs, scratch = refs[:-1], refs[-1]
    scratch[...] = arrived[...].astype(F32)
    owner_row = owner[...].astype(F32)
    at = (iota((tiles, tiles), 0) + first[0]) % tiles
    place = as_column(places(owner_row), tiles, at)
    named = as_column(owner_row, tiles, at) == iota((tiles, peers), 1).astype(F32)
    hot = jnp.concatenate([jnp.where(named & (place == float(slot)), 1.0, 0.0) for slot in range(2)], axis=1)
    rows = jnp.concatenate([take(scratch, peers, 6 * slot, 6) for slot in range(2)], axis=0)
    picked = exact_dot(hot, rows)
    each = tiles // blocks
    for n, out in enumerate(outs):
        out[...] = picked[n * each : (n + 1) * each, :].astype(BF16)


def project_kernel(place, *refs, blocks, tile_rows, slabs):
    moved, coeffs = refs[:blocks], refs[blocks : 2 * blocks]
    near, far, out, wide, weight, sems = refs[2 * blocks :]
    step = pl.program_id(0)
    rows, cols = moved[0].shape
    tiles = rows // tile_rows
    slab = near.shape[0] // (slabs * blocks)

    def weight_copies():
        copies = []
        for e in range(slabs):
            first = lax.rem(place[1] + slabs - e, slabs) * 2
            for n in range(blocks):
                for which, (source, core) in enumerate(((near, place[2]), (far, 1 - place[2]))):
                    at = pl.multiple_of(n * cols + (first + core) * slab, slab)
                    copies.append(
                        pltpu.make_async_copy(
                            source.at[pl.ds((e * blocks + n) * slab, slab), :],
                            weight.at[pl.ds(at, slab), :],
                            sems.at[(e * blocks + n) * 2 + which],
                        )
                    )
        return copies

    @pl.when(step == 0)
    def _():
        copies = weight_copies()
        for copy in copies:
            copy.start()
        for n in range(blocks):
            wide[n] = coeffs[n][...].astype(F32)
        for copy in copies:
            copy.wait()

    strips = []
    for t in range(tiles):
        parts = []
        for n in range(blocks):
            row = wide[n, pl.ds(step * tiles + t, 1), :]
            value = moved[n][t * tile_rows : (t + 1) * tile_rows, :].astype(F32)
            scored = value * row[:, :cols] + (row[:, cols : 2 * cols] + row[:, 2 * cols :])
            parts.append(scored.astype(BF16))
        strips.append(jnp.concatenate(parts, axis=1))
    out[...] = jnp.dot(jnp.concatenate(strips, axis=0), weight[...], preferred_element_type=F32).astype(BF16)


def hop(value, axis, distance):
    size = lax.axis_size(axis)
    return lax.ppermute(value, axis, [(i, (i + distance) % size) for i in range(size)])


def whole(*shape):
    return pl.BlockSpec(shape, lambda *_: (0,) * len(shape))


IN_VMEM = pl.BlockSpec(memory_space=pltpu.VMEM)
IN_SMEM = pl.BlockSpec(memory_space=pltpu.SMEM)
IN_HBM = pl.BlockSpec(memory_space=pltpu.HBM)


def limit(mib):
    return pltpu.CompilerParams(vmem_limit_bytes=mib * MIB)


def held(value):
    return pltpu.with_memory_space_constraint(value, pltpu.VMEM)


def off_chip(value):
    return pltpu.with_memory_space_constraint(value, pltpu.HBM)


def cut(start, sources, rows, on_chip_from=0):
    kept = [pltpu.HBM] * on_chip_from + [pltpu.VMEM] * (len(sources) - on_chip_from)
    return pl.pallas_call(
        lambda *refs: cut_kernel(*refs, count=len(sources), rows=rows),
        in_specs=[IN_SMEM] + [IN_HBM] * len(sources),
        out_specs=[pl.BlockSpec(memory_space=k) for k in kept],
        out_shape=[k((r, s.shape[1]), s.dtype) for k, r, s in zip(kept, rows, sources)],
        scratch_shapes=[pltpu.SemaphoreType.DMA((len(sources),))],
        compiler_params=limit(6),
    )(start, *[off_chip(source) for source in sources])


def stacked(parts):
    rows, cols = parts[0].shape
    return pl.pallas_call(
        stack_kernel,
        in_specs=[pl.BlockSpec(memory_space=pl.ANY)] * len(parts),
        out_specs=IN_HBM,
        out_shape=pltpu.HBM((len(parts) * rows, cols), parts[0].dtype),
        scratch_shapes=[pltpu.SemaphoreType.DMA((len(parts),))],
        compiler_params=limit(6),
    )(*parts)


def on_device(values, subgroup, owners, col_gain, col_bias, out_weight):
    rows, cols = values.shape
    tiles = subgroup.shape[0]
    tile_rows = rows // tiles
    peers, blocks = lax.axis_size("shuf"), lax.axis_size("rep")
    rank, index = lax.axis_index("rep"), lax.axis_index("shuf")
    own_rows = rows // blocks
    outputs = out_weight.shape[1]
    owner_row, sub_row = owners.reshape(1, tiles), subgroup.reshape(1, tiles)

    slabs = 4
    depth = peers // (2 * slabs)
    slab_at, core = index // (2 * depth), index % 2
    slab = cols // (2 * slabs)

    def along_slabs(value, e):
        pairs = [(i, (i + e * 2 * depth) % peers) for i in range(peers)]
        return lax.ppermute(value, "shuf", pairs)

    def quarter(d):
        return ((rank + d) % blocks) * own_rows

    moved = {}
    (two,) = cut(quarter(2).reshape(1), [values], [own_rows], 1)
    moved[2] = hop(two, "rep", 2)

    steps = 4
    outgoing = pl.pallas_call(
        lambda *refs: stats_kernel(*refs, tiles=tiles, peers=peers),
        grid=(steps,),
        in_specs=[
            pl.BlockSpec((rows // steps, cols), lambda i: (i, 0)),
            whole(1, tiles),
            whole(1, tiles),
        ],
        out_specs=whole(peers * MSG, LANES),
        out_shape=jax.ShapeDtypeStruct((peers * MSG, LANES), BF16),
        scratch_shapes=[
            pltpu.VMEM((cols // LANES, tiles * 8, LANES), F32),
            pltpu.VMEM((cols // LANES, tiles * 8, LANES), F32),
            pltpu.VMEM((peers * MSG, LANES), F32),
        ],
        compiler_params=limit(8),
        name="stats",
    )(off_chip(values), owner_row, sub_row)

    def exchange(message):
        arrived = lax.all_to_all(message.reshape(peers, MSG, LANES), "shuf", 0, 0, tiled=True)
        return held(arrived.reshape(peers * MSG, LANES))

    arrived = exchange(outgoing)

    start = jnp.stack([(slab_at * 2 + core) * slab, quarter(1), quarter(3)])
    own_slab, one, three = cut(start, [out_weight, values, values], [slab, own_rows, own_rows])
    slab_parts = [own_slab]
    for d in range(1, blocks):
        slab_parts.append(hop(own_slab, "rep", d))
    moved[1] = hop(one, "rep", 1)
    moved[3] = hop(three, "rep", 3)

    both = pl.pallas_call(
        pair_kernel,
        out_shape=jax.ShapeDtypeStruct((2, cols), F32),
        compiler_params=limit(1),
        name="pair",
    )(col_gain.reshape(1, cols), col_bias.reshape(1, cols))
    answer = pl.pallas_call(
        lambda *refs: owner_kernel(*refs, peers=peers, tile_rows=tile_rows),
        in_specs=[IN_VMEM, whole(2, cols)],
        out_shape=jax.ShapeDtypeStruct((peers * MSG, LANES), BF16),
        scratch_shapes=[pltpu.VMEM((peers * MSG, LANES), F32)],
        compiler_params=limit(6),
        name="moments",
    )(arrived, both)
    returned = exchange(answer)

    one_slab = stacked(slab_parts)
    across = [one_slab]
    for e in range(1, slabs):
        across.append(along_slabs(one_slab, e))
    near = stacked(across)
    far = lax.ppermute(near, "shuf", [(i, i ^ 1) for i in range(peers)])

    each = tiles // blocks
    coeffs = pl.pallas_call(
        lambda *refs: tile_kernel(*refs, tiles=tiles, peers=peers, blocks=blocks),
        in_specs=[IN_SMEM, IN_VMEM, whole(1, tiles)],
        out_specs=[IN_VMEM] * blocks,
        out_shape=[pltpu.VMEM((each, 3 * cols), BF16)] * blocks,
        scratch_shapes=[pltpu.VMEM((peers * MSG, LANES), F32)],
        compiler_params=limit(4),
        name="pick",
    )((rank * each).reshape(1), returned, owner_row)
    known = {0: coeffs[0]}
    for d in (2, 1, 3):
        known[d] = hop(coeffs[d], "rep", d)

    block = min(512, own_rows)
    blocked = pl.BlockSpec((block, cols), lambda i, place: (i, 0))
    return pl.pallas_call(
        lambda *refs: project_kernel(*refs, blocks=blocks, tile_rows=tile_rows, slabs=slabs),
        grid_spec=pltpu.PrefetchScalarGridSpec(
            num_scalar_prefetch=1,
            grid=(own_rows // block,),
            in_specs=[pl.BlockSpec((block, cols), lambda i, place: (place[0] * (own_rows // block) + i, 0))]
            + [blocked] * (blocks - 1)
            + [IN_VMEM] * blocks
            + [IN_HBM] * 2,
            out_specs=pl.BlockSpec((block, outputs), lambda i, place: (i, 0)),
            scratch_shapes=[
                pltpu.VMEM((blocks, each, 3 * cols), F32),
                pltpu.VMEM((blocks * cols, outputs), BF16),
                pltpu.SemaphoreType.DMA((2 * slabs * blocks,)),
            ],
        ),
        out_shape=jax.ShapeDtypeStruct((own_rows, outputs), BF16),
        compiler_params=limit(24),
        name="project",
    )(
        jnp.stack([rank, slab_at, core]),
        off_chip(values),
        *[off_chip(moved[d]) for d in range(1, blocks)],
        *[held(known[d]) for d in range(blocks)],
        off_chip(near),
        off_chip(far),
    )


def solution(mesh):
    return jax.shard_map(
        on_device,
        mesh=mesh,
        in_specs=(P("shuf", "rep"), P("shuf"), P("shuf", None), P("rep"), P("rep"), P("rep", None)),
        out_specs=P(("shuf", "rep"), None),
        check_vma=False,
    )
```

```python
import jax
import jax.numpy as jnp
from jax import lax
from jax.experimental import pallas as pl
from jax.experimental.pallas import tpu as pltpu
from jax.sharding import PartitionSpec as P

GRP_DEV = 32
PRIOR = 256.0
LANES = 128
MSG = 16
F32 = jnp.float32
BF16 = jnp.bfloat16
MIB = 1 << 20


def iota(shape, dim):
    return lax.broadcasted_iota(jnp.int32, shape, dim)


def exact_dot(one_hot, rows):
    return jnp.dot(one_hot.astype(BF16), rows.astype(BF16), preferred_element_type=F32)


def as_column(row, size, at):
    picked = jnp.where(at == iota((size, size), 1), jnp.broadcast_to(row, (size, size)), 0.0)
    return jnp.sum(picked, axis=1, keepdims=True)


def places(owner_row):
    size = owner_row.shape[1]
    column = as_column(owner_row, size, iota((size, size), 0))
    same = column == jnp.broadcast_to(owner_row, (size, size))
    earlier = iota((size, size), 0) < iota((size, size), 1)
    return jnp.sum(jnp.where(same & earlier, 1.0, 0.0), axis=0, keepdims=True)


def put(scratch, part, peers, at):
    for n in range(part.shape[1] // LANES):
        scratch[pl.ds(at + n, peers, stride=MSG), :] = part[:, n * LANES : (n + 1) * LANES]


def take(scratch, peers, at, count):
    return jnp.concatenate([scratch[pl.ds(at + n, peers, stride=MSG), :] for n in range(count)], axis=1)


def run(copies):
    for copy in copies:
        copy.start()
    for copy in copies:
        copy.wait()


def row_copies(starts, sources, outs, sems, rows):
    return [
        pltpu.make_async_copy(source.at[pl.ds(pl.multiple_of(start, rows), rows), :], out, sems.at[n])
        for n, (start, source, out) in enumerate(zip(starts, sources, outs))
    ]


def cut_kernel(info, source, out, sems, *, rows, start):
    run(row_copies([start(info)], [source], [out], sems, rows))


def cut13_kernel(info, values, *refs, rows, blocks, pieces):
    outs, held_rows, sems_in, sems_out = refs[:2], refs[2], refs[3], refs[4]
    size = rows // pieces
    inward, outward = [], []
    for q, d in enumerate((1, 3)):
        for p in range(pieces):
            n = q * pieces + p
            at = pl.multiple_of(lax.rem(info[0] + d, blocks) * rows + p * size, size)
            inward.append(pltpu.make_async_copy(values.at[pl.ds(at, size), :], held_rows.at[n], sems_in.at[n]))
            outward.append(pltpu.make_async_copy(held_rows.at[n], outs[q].at[pl.ds(p * size, size), :], sems_out.at[n]))
    for copy in inward:
        copy.start()
    for copy, onward in zip(inward, outward):
        copy.wait()
        onward.start()
    for onward in outward:
        onward.wait()


def stack_kernel(*refs):
    parts, out, sems = refs[:-2], refs[-2], refs[-1]
    rows = parts[0].shape[0]
    run(
        [
            pltpu.make_async_copy(part, out.at[n * rows : (n + 1) * rows, :], sems.at[n])
            for n, part in enumerate(parts)
        ]
    )


def assemble_kernel(info, *refs, blocks, slabs, cols):
    parts, out, sems = refs[: 2 * slabs], refs[-2], refs[-1]
    slab = parts[0].shape[0] // blocks
    copies = []
    for e in range(slabs):
        first = lax.rem(info[1] + slabs - e, slabs) * 2
        for c in range(2):
            number = first + (info[2] if c == 0 else 1 - info[2])
            for n in range(blocks):
                at = pl.multiple_of(n * cols + number * slab, slab)
                source = parts[2 * e + c].at[pl.ds(n * slab, slab), :]
                copies.append(pltpu.make_async_copy(source, out.at[pl.ds(at, slab), :], sems.at[len(copies)]))
    run(copies)


def stats_kernel(values, owner, sub, out, first, second, scratch, *, tiles, peers):
    step = pl.program_id(0)
    rows, cols = values.shape
    here = tiles // pl.num_programs(0)
    tile_rows = rows // here
    chunk = 16

    def one_tile(t, carry):
        low = high = None
        for n in range(tile_rows // chunk):
            at = pl.multiple_of(t * tile_rows + n * chunk, chunk)
            wide = values[pl.ds(at, chunk), :].astype(F32)
            low, high = (wide, wide * wide) if low is None else (low + wide, high + wide * wide)
        at = pl.multiple_of((step * here + t) * 8, 8)
        for n in range(cols // LANES):
            lanes = slice(n * LANES, (n + 1) * LANES)
            first[n, pl.ds(at, 8), :] = low[:8, lanes] + low[8:, lanes]
            second[n, pl.ds(at, 8), :] = high[:8, lanes] + high[8:, lanes]
        return carry

    lax.fori_loop(0, here, one_tile, 0, unroll=2)

    @pl.when(step == pl.num_programs(0) - 1)
    def _():
        def folded(ref):
            halves = []
            for n in range(cols // LANES):
                rows = [ref[n, pl.ds(r, tiles, stride=8), :] for r in range(8)]
                while len(rows) > 1:
                    rows = [a + b for a, b in zip(rows[::2], rows[1::2])]
                halves.append(rows[0])
            return jnp.concatenate(halves, axis=1) * (1.0 / tile_rows)

        all_mean = folded(first)
        all_var = folded(second) - all_mean * all_mean
        dev_mean = jnp.sum(all_mean, axis=0, keepdims=True) * (1.0 / tiles)
        apart = all_mean - dev_mean
        dev_var = jnp.sum(all_var + apart * apart, axis=0, keepdims=True) * (1.0 / tiles)
        owner_row = owner[...].astype(F32)
        place = places(owner_row)
        named = jnp.broadcast_to(owner_row, (peers, tiles)) == iota((peers, tiles), 0).astype(F32)
        sub_column = as_column(sub[...].astype(F32), tiles, iota((tiles, tiles), 0))
        sub_wide = jnp.broadcast_to(sub_column + 1.0, (tiles, LANES))
        hot = jnp.concatenate([jnp.where(named & (place == float(slot)), 1.0, 0.0) for slot in range(2)], axis=0)
        sent = exact_dot(hot, jnp.concatenate([all_mean, all_var, sub_wide], axis=1))
        for slot in range(2):
            here = sent[slot * peers : (slot + 1) * peers, :]
            put(scratch, here[:, : 2 * cols], peers, 4 * slot)
            put(scratch, here[:, 2 * cols :] - 1.0, peers, 14 + slot)
        high = dev_mean.astype(BF16).astype(F32)
        put(scratch, jnp.broadcast_to(high, (peers, cols)), peers, 8)
        put(scratch, jnp.broadcast_to(dev_mean - high, (peers, cols)), peers, 10)
        put(scratch, jnp.broadcast_to(dev_var, (peers, cols)), peers, 12)
        out[...] = scratch[...].astype(BF16)


def pair_kernel(gain, bias, out):
    out[0:1, :] = gain[...]
    out[1:2, :] = bias[...]


def owner_kernel(arrived, both, out, scratch, *, peers, tile_rows):
    scratch[...] = arrived[...].astype(F32)
    dev_mean = take(scratch, peers, 8, 2) + take(scratch, peers, 10, 2)
    mean_all = jnp.sum(dev_mean, axis=0, keepdims=True) * (1.0 / peers)
    apart = dev_mean - mean_all
    var_all = jnp.sum(take(scratch, peers, 12, 2) + apart * apart, axis=0, keepdims=True) * (1.0 / peers)
    cols = dev_mean.shape[1]
    forth, back, firsts, seconds = [], [], [], []
    for slot in range(2):
        label = take(scratch, peers, 14 + slot, 1)
        back.append(jnp.where(label[:, :GRP_DEV] == iota((peers, GRP_DEV), 1).astype(F32), 1.0, 0.0))
        on_diagonal = iota((peers, peers), 0) == iota((peers, peers), 1)
        row = jnp.sum(jnp.where(on_diagonal, label[:, :peers], 0.0), axis=0, keepdims=True)
        wide = jnp.broadcast_to(row, (GRP_DEV, peers))
        forth.append(jnp.where(wide == iota((GRP_DEV, peers), 0).astype(F32), 1.0, 0.0))
        shifted = take(scratch, peers, 4 * slot, 2) - mean_all
        firsts.append(shifted)
        seconds.append(take(scratch, peers, 4 * slot + 2, 2) + shifted * shifted)
    forth = jnp.concatenate(forth, axis=1)
    count = jnp.sum(forth, axis=1, keepdims=True) * float(tile_rows)
    data = jnp.concatenate([jnp.concatenate(firsts, axis=0), jnp.concatenate(seconds, axis=0)], axis=1)
    high = data.astype(BF16).astype(F32)
    middle = (data - high).astype(BF16).astype(F32)
    parts = exact_dot(forth, jnp.concatenate([high, middle, data - high - middle], axis=1))
    sums = (parts[:, : 2 * cols] + parts[:, 2 * cols : 4 * cols] + parts[:, 4 * cols :]) * float(tile_rows)
    portion = 1.0 / (count + PRIOR)
    center = sums[:, :cols] * portion
    second = (sums[:, cols:] + PRIOR * var_all) * portion
    inverse = lax.rsqrt(second - center * center + 1e-05)
    scale = (inverse * both[0:1, :]).astype(BF16).astype(F32)
    shift = both[1:2, :] - (center + mean_all) * scale
    shift_high = shift.astype(BF16).astype(F32)
    reply = exact_dot(
        jnp.concatenate(back, axis=0), jnp.concatenate([scale, shift_high, shift - shift_high], axis=1)
    )
    for slot in range(2):
        put(scratch, reply[slot * peers : (slot + 1) * peers, :], peers, 6 * slot)
    out[...] = scratch[...].astype(BF16)


def tile_kernel(info, arrived, owner, *refs, tiles, peers, blocks):
    outs, scratch = refs[:-1], refs[-1]
    scratch[...] = arrived[...].astype(F32)
    owner_row = owner[...].astype(F32)
    at = (iota((tiles, tiles), 0) + info[0] * (tiles // blocks)) % tiles
    place = as_column(places(owner_row), tiles, at)
    named = as_column(owner_row, tiles, at) == iota((tiles, peers), 1).astype(F32)
    hot = jnp.concatenate([jnp.where(named & (place == float(slot)), 1.0, 0.0) for slot in range(2)], axis=1)
    rows = jnp.concatenate([take(scratch, peers, 6 * slot, 6) for slot in range(2)], axis=0)
    picked = exact_dot(hot, rows)
    each = tiles // blocks
    for n, out in enumerate(outs):
        out[...] = picked[n * each : (n + 1) * each, :].astype(BF16)


def project_kernel(info, *refs, blocks, tile_rows):
    moved, coeffs, (weight, out, wide) = refs[:blocks], refs[blocks : 2 * blocks], refs[2 * blocks :]
    step = pl.program_id(0)
    rows, cols = moved[0].shape
    tiles = rows // tile_rows

    @pl.when(step == 0)
    def _():
        for n in range(blocks):
            wide[n] = coeffs[n][...].astype(F32)

    strips = []
    for t in range(tiles):
        parts = []
        for n in range(blocks):
            row = wide[n, pl.ds(step * tiles + t, 1), :]
            value = moved[n][t * tile_rows : (t + 1) * tile_rows, :].astype(F32)
            scored = value * row[:, :cols] + (row[:, cols : 2 * cols] + row[:, 2 * cols :])
            parts.append(scored.astype(BF16))
        strips.append(jnp.concatenate(parts, axis=1))
    out[...] = jnp.dot(jnp.concatenate(strips, axis=0), weight[...], preferred_element_type=F32).astype(BF16)


def hop(value, axis, distance):
    size = lax.axis_size(axis)
    return lax.ppermute(value, axis, [(i, (i + distance) % size) for i in range(size)])


def whole(*shape):
    return pl.BlockSpec(shape, lambda *_: (0,) * len(shape))


IN_VMEM = pl.BlockSpec(memory_space=pltpu.VMEM)
IN_SMEM = pl.BlockSpec(memory_space=pltpu.SMEM)
IN_HBM = pl.BlockSpec(memory_space=pltpu.HBM)


def limit(mib):
    return pltpu.CompilerParams(vmem_limit_bytes=mib * MIB)


def held(value):
    return pltpu.with_memory_space_constraint(value, pltpu.VMEM)


def off_chip(value):
    return pltpu.with_memory_space_constraint(value, pltpu.HBM)


IN_ANY = pl.BlockSpec(memory_space=pl.ANY)


def cut(info, source, rows, start):
    return pl.pallas_call(
        lambda *refs: cut_kernel(*refs, rows=rows, start=start),
        in_specs=[IN_SMEM, IN_HBM],
        out_specs=IN_VMEM,
        out_shape=pltpu.VMEM((rows, source.shape[1]), source.dtype),
        scratch_shapes=[pltpu.SemaphoreType.DMA((1,))],
        compiler_params=limit(2),
    )(info, off_chip(source))


def stacked(parts):
    rows, cols = parts[0].shape
    return pl.pallas_call(
        stack_kernel,
        in_specs=[IN_VMEM] * len(parts),
        out_specs=IN_VMEM,
        out_shape=pltpu.VMEM((len(parts) * rows, cols), parts[0].dtype),
        scratch_shapes=[pltpu.SemaphoreType.DMA((len(parts),))],
        compiler_params=limit(2),
    )(*[held(part) for part in parts])


def on_device(values, subgroup, owners, col_gain, col_bias, out_weight):
    rows, cols = values.shape
    tiles = subgroup.shape[0]
    tile_rows = rows // tiles
    peers, blocks = lax.axis_size("shuf"), lax.axis_size("rep")
    rank, index = lax.axis_index("rep"), lax.axis_index("shuf")
    own_rows = rows // blocks
    outputs = out_weight.shape[1]
    owner_row, sub_row = owners.reshape(1, tiles), subgroup.reshape(1, tiles)

    slabs = 2
    depth = max(1, peers // 8)
    info = jnp.stack([rank, (index // (2 * depth)) % slabs, index % 2])
    slab = cols // (2 * slabs)

    def trade(value, distance):
        return lax.ppermute(value, "shuf", [(i, i ^ distance) for i in range(peers)])

    moved = {}
    two = cut(info, values, own_rows, lambda ref: lax.rem(ref[0] + 2, blocks) * own_rows)
    moved[2] = hop(two, "rep", 2)

    steps = 4
    outgoing = pl.pallas_call(
        lambda *refs: stats_kernel(*refs, tiles=tiles, peers=peers),
        grid=(steps,),
        in_specs=[
            pl.BlockSpec((rows // steps, cols), lambda i: (i, 0)),
            whole(1, tiles),
            whole(1, tiles),
        ],
        out_specs=whole(peers * MSG, LANES),
        out_shape=jax.ShapeDtypeStruct((peers * MSG, LANES), BF16),
        scratch_shapes=[
            pltpu.VMEM((cols // LANES, tiles * 8, LANES), F32),
            pltpu.VMEM((cols // LANES, tiles * 8, LANES), F32),
            pltpu.VMEM((peers * MSG, LANES), F32),
        ],
        compiler_params=limit(8),
        name="stats",
    )(off_chip(values), owner_row, sub_row)

    def exchange(message):
        arrived = lax.all_to_all(message.reshape(peers, MSG, LANES), "shuf", 0, 0, tiled=True)
        return held(arrived.reshape(peers * MSG, LANES))

    arrived = exchange(outgoing)

    own_slab = cut(info, out_weight, slab, lambda ref: (ref[1] * 2 + ref[2]) * slab)
    slab_parts = [own_slab]
    for d in range(1, blocks):
        slab_parts.append(hop(own_slab, "rep", d))
    pieces = 4
    one, three = pl.pallas_call(
        lambda *refs: cut13_kernel(*refs, rows=own_rows, blocks=blocks, pieces=pieces),
        in_specs=[IN_SMEM, IN_HBM],
        out_specs=[IN_HBM] * 2,
        out_shape=[pltpu.HBM((own_rows, cols), BF16)] * 2,
        scratch_shapes=[
            pltpu.VMEM((2 * pieces, own_rows // pieces, cols), BF16),
            pltpu.SemaphoreType.DMA((2 * pieces,)),
            pltpu.SemaphoreType.DMA((2 * pieces,)),
        ],
        compiler_params=limit(4),
        name="cut13",
    )(info, off_chip(values))
    moved[1] = hop(one, "rep", 1)
    moved[3] = hop(three, "rep", 3)

    both = pl.pallas_call(
        pair_kernel,
        out_shape=jax.ShapeDtypeStruct((2, cols), F32),
        compiler_params=limit(1),
        name="pair",
    )(col_gain.reshape(1, cols), col_bias.reshape(1, cols))
    answer = pl.pallas_call(
        lambda *refs: owner_kernel(*refs, peers=peers, tile_rows=tile_rows),
        in_specs=[IN_VMEM, whole(2, cols)],
        out_shape=jax.ShapeDtypeStruct((peers * MSG, LANES), BF16),
        scratch_shapes=[pltpu.VMEM((peers * MSG, LANES), F32)],
        compiler_params=limit(6),
        name="moments",
    )(arrived, both)
    returned = exchange(answer)

    parts = [stacked(slab_parts)]
    parts.append(trade(parts[0], 1))
    parts.append(trade(parts[0], 2 * depth))
    parts.append(trade(parts[2], 1))
    weight = pl.pallas_call(
        lambda *refs: assemble_kernel(*refs, blocks=blocks, slabs=slabs, cols=cols),
        in_specs=[IN_SMEM] + [IN_ANY] * len(parts),
        out_specs=IN_VMEM,
        out_shape=pltpu.VMEM((blocks * cols, outputs), BF16),
        scratch_shapes=[pltpu.SemaphoreType.DMA((2 * slabs * blocks,))],
        compiler_params=limit(2),
        name="assemble",
    )(info, *parts)

    each = tiles // blocks
    coeffs = pl.pallas_call(
        lambda *refs: tile_kernel(*refs, tiles=tiles, peers=peers, blocks=blocks),
        in_specs=[IN_SMEM, IN_VMEM, whole(1, tiles)],
        out_specs=[IN_VMEM] * blocks,
        out_shape=[pltpu.VMEM((each, 3 * cols), BF16)] * blocks,
        scratch_shapes=[pltpu.VMEM((peers * MSG, LANES), F32)],
        compiler_params=limit(4),
        name="pick",
    )(info, returned, owner_row)
    known = {0: coeffs[0]}
    for d in (2, 1, 3):
        known[d] = hop(coeffs[d], "rep", d)

    block = min(512, own_rows)
    return pl.pallas_call(
        lambda *refs: project_kernel(*refs, blocks=blocks, tile_rows=tile_rows),
        grid_spec=pltpu.PrefetchScalarGridSpec(
            num_scalar_prefetch=1,
            grid=(own_rows // block,),
            in_specs=[pl.BlockSpec((block, cols), lambda i, info: (info[0] * (own_rows // block) + i, 0))]
            + [pl.BlockSpec((block, cols), lambda i, info: (i, 0))] * (blocks - 1)
            + [IN_VMEM] * (blocks + 1),
            out_specs=pl.BlockSpec((block, outputs), lambda i, info: (i, 0)),
            scratch_shapes=[pltpu.VMEM((blocks, each, 3 * cols), F32)],
        ),
        out_shape=jax.ShapeDtypeStruct((own_rows, outputs), BF16),
        compiler_params=limit(24),
        name="project",
    )(
        info,
        off_chip(values),
        *[off_chip(moved[d]) for d in range(1, blocks)],
        *[held(known[d]) for d in range(blocks)],
        held(weight),
    )


def solution(mesh):
    return jax.shard_map(
        on_device,
        mesh=mesh,
        in_specs=(P("shuf", "rep"), P("shuf"), P("shuf", None), P("rep"), P("rep"), P("rep", None)),
        out_specs=P(("shuf", "rep"), None),
        check_vma=False,
    )
```

```python
import jax
import jax.numpy as jnp
from jax import lax
from jax.experimental import pallas as pl
from jax.experimental.pallas import tpu as pltpu
from jax.sharding import PartitionSpec as P


GRP_DEV = 32
PRIOR = 256.0
LANES = 128
MSG = 16
F32 = jnp.float32
BF16 = jnp.bfloat16
MIB = 1 << 20


def iota(shape, dim):
    return lax.broadcasted_iota(jnp.int32, shape, dim)


def exact_dot(one_hot, rows):
    return jnp.dot(one_hot.astype(BF16), rows.astype(BF16), preferred_element_type=F32)


def as_column(row, size, at):
    picked = jnp.where(at == iota((size, size), 1), jnp.broadcast_to(row, (size, size)), 0.0)
    return jnp.sum(picked, axis=1, keepdims=True)


def places(owner_row):
    size = owner_row.shape[1]
    column = as_column(owner_row, size, iota((size, size), 0))
    same = column == jnp.broadcast_to(owner_row, (size, size))
    earlier = iota((size, size), 0) < iota((size, size), 1)
    return jnp.sum(jnp.where(same & earlier, 1.0, 0.0), axis=0, keepdims=True)


def put(scratch, part, peers, at):
    for n in range(part.shape[1] // LANES):
        scratch[pl.ds(at + n, peers, stride=MSG), :] = part[:, n * LANES : (n + 1) * LANES]


def take(scratch, peers, at, count):
    return jnp.concatenate([scratch[pl.ds(at + n, peers, stride=MSG), :] for n in range(count)], axis=1)


def run(copies):
    for copy in copies:
        copy.start()
    for copy in copies:
        copy.wait()


def row_copies(starts, sources, outs, sems, rows):
    return [
        pltpu.make_async_copy(source.at[pl.ds(pl.multiple_of(start, rows), rows), :], out, sems.at[n])
        for n, (start, source, out) in enumerate(zip(starts, sources, outs))
    ]


def cut_kernel(info, values, weight, out_rows, out_slab, sems, *, rows, slab, blocks):
    run(
        row_copies([info[2] * slab], [weight], [out_slab], sems, slab)
        + row_copies([lax.rem(info[0] + 2, blocks) * rows], [values], [out_rows], sems.at[1:], rows)
    )


def stack_kernel(*refs):
    parts, out = refs[:-1], refs[-1]
    rows = parts[0].shape[0]
    for n, part in enumerate(parts):
        out[n * rows : (n + 1) * rows, :] = part[...]


def assemble_kernel(info, near, far, out, sems, *, blocks, cols):
    half = near.shape[0] // blocks

    def rows_of(n, number):
        return out.at[pl.ds(pl.multiple_of(n * cols + number * half, half), half), :]

    copies = [
        pltpu.make_async_copy(near.at[pl.ds(n * half, half), :], rows_of(n, info[2]), sems.at[n])
        for n in range(blocks)
    ]
    for copy in copies:
        copy.start()
    for n in range(blocks):
        rows_of(n, 1 - info[2])[...] = far[n * half : (n + 1) * half, :]
    for copy in copies:
        copy.wait()


def quarter_of(step, rank, blocks):
    return lax.rem(rank + jnp.where(step == 0, 1, jnp.where(step == 1, 3, jnp.where(step == 2, 0, 2))), blocks)


def stats_kernel(info, values, owner, sub, out, one, three, first, second, scratch, sems, *, tiles, peers):
    step = pl.program_id(0)
    rows, cols = values.shape
    blocks = 4
    here = tiles // blocks
    quarter = quarter_of(step, info[0], blocks)
    for n, sent in enumerate((one, three)):

        @pl.when(step == n)
        def _():
            pltpu.make_async_copy(values, sent, sems.at[n]).start()

    tile_rows = rows // here
    chunk = 16

    def one_tile(t, carry):
        low = high = None
        for n in range(tile_rows // chunk):
            at = pl.multiple_of(t * tile_rows + n * chunk, chunk)
            wide = values[pl.ds(at, chunk), :].astype(F32)
            low, high = (wide, wide * wide) if low is None else (low + wide, high + wide * wide)
        at = pl.multiple_of((quarter * here + t) * 8, 8)
        for n in range(cols // LANES):
            lanes = slice(n * LANES, (n + 1) * LANES)
            first[n, pl.ds(at, 8), :] = low[:8, lanes] + low[8:, lanes]
            second[n, pl.ds(at, 8), :] = high[:8, lanes] + high[8:, lanes]
        return carry

    lax.fori_loop(0, here, one_tile, 0, unroll=2)
    for n, sent in enumerate((one, three)):

        @pl.when(step == n)
        def _():
            pltpu.make_async_copy(values, sent, sems.at[n]).wait()

    @pl.when(step == pl.num_programs(0) - 1)
    def _():
        def folded(ref):
            halves = []
            for n in range(cols // LANES):
                rows = [ref[n, pl.ds(r, tiles, stride=8), :] for r in range(8)]
                while len(rows) > 1:
                    rows = [a + b for a, b in zip(rows[::2], rows[1::2])]
                halves.append(rows[0])
            return jnp.concatenate(halves, axis=1) * (1.0 / tile_rows)

        all_mean = folded(first)
        all_var = folded(second) - all_mean * all_mean
        dev_mean = jnp.sum(all_mean, axis=0, keepdims=True) * (1.0 / tiles)
        apart = all_mean - dev_mean
        dev_var = jnp.sum(all_var + apart * apart, axis=0, keepdims=True) * (1.0 / tiles)
        owner_row = owner[...].astype(F32)
        place = places(owner_row)
        named = jnp.broadcast_to(owner_row, (peers, tiles)) == iota((peers, tiles), 0).astype(F32)
        sub_column = as_column(sub[...].astype(F32), tiles, iota((tiles, tiles), 0))
        sub_wide = jnp.broadcast_to(sub_column + 1.0, (tiles, LANES))
        hot = jnp.concatenate([jnp.where(named & (place == float(slot)), 1.0, 0.0) for slot in range(2)], axis=0)
        sent = exact_dot(hot, jnp.concatenate([all_mean, all_var, sub_wide], axis=1))
        for slot in range(2):
            here = sent[slot * peers : (slot + 1) * peers, :]
            put(scratch, here[:, : 2 * cols], peers, 4 * slot)
            put(scratch, here[:, 2 * cols :] - 1.0, peers, 14 + slot)
        high = dev_mean.astype(BF16).astype(F32)
        put(scratch, jnp.broadcast_to(high, (peers, cols)), peers, 8)
        put(scratch, jnp.broadcast_to(dev_mean - high, (peers, cols)), peers, 10)
        put(scratch, jnp.broadcast_to(dev_var, (peers, cols)), peers, 12)
        out[...] = scratch[...].astype(BF16)


def pair_kernel(gain, bias, out):
    out[0:1, :] = gain[...]
    out[1:2, :] = bias[...]


def owner_kernel(arrived, both, out, scratch, *, peers, tile_rows):
    scratch[...] = arrived[...].astype(F32)
    dev_mean = take(scratch, peers, 8, 2) + take(scratch, peers, 10, 2)
    mean_all = jnp.sum(dev_mean, axis=0, keepdims=True) * (1.0 / peers)
    apart = dev_mean - mean_all
    var_all = jnp.sum(take(scratch, peers, 12, 2) + apart * apart, axis=0, keepdims=True) * (1.0 / peers)
    cols = dev_mean.shape[1]
    forth, back, firsts, seconds = [], [], [], []
    for slot in range(2):
        label = take(scratch, peers, 14 + slot, 1)
        back.append(jnp.where(label[:, :GRP_DEV] == iota((peers, GRP_DEV), 1).astype(F32), 1.0, 0.0))
        on_diagonal = iota((peers, peers), 0) == iota((peers, peers), 1)
        row = jnp.sum(jnp.where(on_diagonal, label[:, :peers], 0.0), axis=0, keepdims=True)
        wide = jnp.broadcast_to(row, (GRP_DEV, peers))
        forth.append(jnp.where(wide == iota((GRP_DEV, peers), 0).astype(F32), 1.0, 0.0))
        shifted = take(scratch, peers, 4 * slot, 2) - mean_all
        firsts.append(shifted)
        seconds.append(take(scratch, peers, 4 * slot + 2, 2) + shifted * shifted)
    forth = jnp.concatenate(forth, axis=1)
    count = jnp.sum(forth, axis=1, keepdims=True) * float(tile_rows)
    data = jnp.concatenate([jnp.concatenate(firsts, axis=0), jnp.concatenate(seconds, axis=0)], axis=1)
    high = data.astype(BF16).astype(F32)
    middle = (data - high).astype(BF16).astype(F32)
    parts = exact_dot(forth, jnp.concatenate([high, middle, data - high - middle], axis=1))
    sums = (parts[:, : 2 * cols] + parts[:, 2 * cols : 4 * cols] + parts[:, 4 * cols :]) * float(tile_rows)
    portion = 1.0 / (count + PRIOR)
    center = sums[:, :cols] * portion
    second = (sums[:, cols:] + PRIOR * var_all) * portion
    inverse = lax.rsqrt(second - center * center + 1e-05)
    scale = (inverse * both[0:1, :]).astype(BF16).astype(F32)
    shift = both[1:2, :] - (center + mean_all) * scale
    shift_high = shift.astype(BF16).astype(F32)
    reply = exact_dot(
        jnp.concatenate(back, axis=0), jnp.concatenate([scale, shift_high, shift - shift_high], axis=1)
    )
    for slot in range(2):
        put(scratch, reply[slot * peers : (slot + 1) * peers, :], peers, 6 * slot)
    out[...] = scratch[...].astype(BF16)


def tile_kernel(info, arrived, owner, *refs, tiles, peers, blocks):
    outs, scratch = refs[:-1], refs[-1]
    scratch[...] = arrived[...].astype(F32)
    owner_row = owner[...].astype(F32)
    at = (iota((tiles, tiles), 0) + info[0] * (tiles // blocks)) % tiles
    place = as_column(places(owner_row), tiles, at)
    named = as_column(owner_row, tiles, at) == iota((tiles, peers), 1).astype(F32)
    hot = jnp.concatenate([jnp.where(named & (place == float(slot)), 1.0, 0.0) for slot in range(2)], axis=1)
    rows = jnp.concatenate([take(scratch, peers, 6 * slot, 6) for slot in range(2)], axis=0)
    picked = exact_dot(hot, rows)
    each = tiles // blocks
    for n, out in enumerate(outs):
        out[...] = picked[n * each : (n + 1) * each, :].astype(BF16)


def project_kernel(info, *refs, blocks, tile_rows):
    moved, coeffs, (weight, out, wide) = refs[:blocks], refs[blocks : 2 * blocks], refs[2 * blocks :]
    step = pl.program_id(0)
    rows, cols = moved[0].shape
    tiles = rows // tile_rows

    @pl.when(step == 0)
    def _():
        for n in range(blocks):
            wide[n] = coeffs[n][...].astype(F32)

    strips = []
    for t in range(tiles):
        parts = []
        for n in range(blocks):
            row = wide[n, pl.ds(step * tiles + t, 1), :]
            value = moved[n][t * tile_rows : (t + 1) * tile_rows, :].astype(F32)
            scored = value * row[:, :cols] + (row[:, cols : 2 * cols] + row[:, 2 * cols :])
            parts.append(scored.astype(BF16))
        strips.append(jnp.concatenate(parts, axis=1))
    out[...] = jnp.dot(jnp.concatenate(strips, axis=0), weight[...], preferred_element_type=F32).astype(BF16)


def hop(value, axis, distance):
    size = lax.axis_size(axis)
    return lax.ppermute(value, axis, [(i, (i + distance) % size) for i in range(size)])


def whole(*shape):
    return pl.BlockSpec(shape, lambda *_: (0,) * len(shape))


IN_VMEM = pl.BlockSpec(memory_space=pltpu.VMEM)
IN_SMEM = pl.BlockSpec(memory_space=pltpu.SMEM)
IN_HBM = pl.BlockSpec(memory_space=pltpu.HBM)


def limit(mib):
    return pltpu.CompilerParams(vmem_limit_bytes=mib * MIB)


def held(value):
    return pltpu.with_memory_space_constraint(value, pltpu.VMEM)


def off_chip(value):
    return pltpu.with_memory_space_constraint(value, pltpu.HBM)


IN_ANY = pl.BlockSpec(memory_space=pl.ANY)


def stacked(parts):
    rows, cols = parts[0].shape
    return pl.pallas_call(
        stack_kernel,
        in_specs=[whole(rows, cols)] * len(parts),
        out_specs=whole(len(parts) * rows, cols),
        out_shape=pltpu.HBM((len(parts) * rows, cols), parts[0].dtype),
        compiler_params=limit(8),
    )(*parts)


def on_device(values, subgroup, owners, col_gain, col_bias, out_weight):
    rows, cols = values.shape
    tiles = subgroup.shape[0]
    tile_rows = rows // tiles
    peers, blocks = lax.axis_size("shuf"), lax.axis_size("rep")
    rank, index = lax.axis_index("rep"), lax.axis_index("shuf")
    own_rows = rows // blocks
    outputs = out_weight.shape[1]
    owner_row, sub_row = owners.reshape(1, tiles), subgroup.reshape(1, tiles)

    info = jnp.stack([rank, index, index % 2])
    slab = cols // 2

    moved = {}
    two, own_slab = pl.pallas_call(
        lambda *refs: cut_kernel(*refs, rows=own_rows, slab=slab, blocks=blocks),
        in_specs=[IN_SMEM, IN_HBM, IN_HBM],
        out_specs=[IN_VMEM] * 2,
        out_shape=[pltpu.VMEM((own_rows, cols), BF16), pltpu.VMEM((slab, outputs), BF16)],
        scratch_shapes=[pltpu.SemaphoreType.DMA((2,))],
        compiler_params=limit(2),
        name="cut",
    )(info, off_chip(values), off_chip(out_weight))
    moved[2] = hop(two, "rep", 2)

    in_order = pl.BlockSpec((own_rows, cols), lambda i, info: (quarter_of(i, info[0], blocks), 0))
    outgoing, one, three = pl.pallas_call(
        lambda *refs: stats_kernel(*refs, tiles=tiles, peers=peers),
        grid_spec=pltpu.PrefetchScalarGridSpec(
            num_scalar_prefetch=1,
            grid=(blocks,),
            in_specs=[in_order, whole(1, tiles), whole(1, tiles)],
            out_specs=[whole(peers * MSG, LANES), IN_HBM, IN_HBM],
            scratch_shapes=[
                pltpu.VMEM((cols // LANES, tiles * 8, LANES), F32),
                pltpu.VMEM((cols // LANES, tiles * 8, LANES), F32),
                pltpu.VMEM((peers * MSG, LANES), F32),
                pltpu.SemaphoreType.DMA((2,)),
            ],
        ),
        out_shape=[jax.ShapeDtypeStruct((peers * MSG, LANES), BF16)]
        + [pltpu.HBM((own_rows, cols), BF16)] * 2,
        compiler_params=limit(8),
        name="stats",
    )(info, off_chip(values), owner_row, sub_row)

    def exchange(message):
        arrived = lax.all_to_all(message.reshape(peers, MSG, LANES), "shuf", 0, 0, tiled=True)
        return held(arrived.reshape(peers * MSG, LANES))

    arrived = exchange(outgoing)

    slab_parts = [own_slab]
    for d in range(1, blocks):
        slab_parts.append(hop(own_slab, "rep", d))
    moved[1] = hop(one, "rep", 1)
    moved[3] = hop(three, "rep", 3)

    both = pl.pallas_call(
        pair_kernel,
        out_shape=jax.ShapeDtypeStruct((2, cols), F32),
        compiler_params=limit(1),
        name="pair",
    )(col_gain.reshape(1, cols), col_bias.reshape(1, cols))
    answer = pl.pallas_call(
        lambda *refs: owner_kernel(*refs, peers=peers, tile_rows=tile_rows),
        in_specs=[IN_VMEM, whole(2, cols)],
        out_shape=jax.ShapeDtypeStruct((peers * MSG, LANES), BF16),
        scratch_shapes=[pltpu.VMEM((peers * MSG, LANES), F32)],
        compiler_params=limit(6),
        name="moments",
    )(arrived, both)
    returned = exchange(answer)

    near = stacked(slab_parts)
    far = lax.ppermute(near, "shuf", [(i, i ^ 1) for i in range(peers)])
    weight = pl.pallas_call(
        lambda *refs: assemble_kernel(*refs, blocks=blocks, cols=cols),
        in_specs=[IN_SMEM, IN_HBM, IN_VMEM],
        out_specs=IN_VMEM,
        out_shape=pltpu.VMEM((blocks * cols, outputs), BF16),
        scratch_shapes=[pltpu.SemaphoreType.DMA((blocks,))],
        compiler_params=limit(2),
        name="assemble",
    )(info, off_chip(near), held(far))

    each = tiles // blocks
    coeffs = pl.pallas_call(
        lambda *refs: tile_kernel(*refs, tiles=tiles, peers=peers, blocks=blocks),
        in_specs=[IN_SMEM, IN_VMEM, whole(1, tiles)],
        out_specs=[IN_VMEM] * blocks,
        out_shape=[pltpu.VMEM((each, 3 * cols), BF16)] * blocks,
        scratch_shapes=[pltpu.VMEM((peers * MSG, LANES), F32)],
        compiler_params=limit(4),
        name="pick",
    )(info, returned, owner_row)
    known = {0: coeffs[0]}
    for d in (2, 1, 3):
        known[d] = hop(coeffs[d], "rep", d)

    block = min(512, own_rows)
    return pl.pallas_call(
        lambda *refs: project_kernel(*refs, blocks=blocks, tile_rows=tile_rows),
        grid_spec=pltpu.PrefetchScalarGridSpec(
            num_scalar_prefetch=1,
            grid=(own_rows // block,),
            in_specs=[pl.BlockSpec((block, cols), lambda i, info: (info[0] * (own_rows // block) + i, 0))]
            + [pl.BlockSpec((block, cols), lambda i, info: (i, 0))] * (blocks - 1)
            + [IN_VMEM] * (blocks + 1),
            out_specs=pl.BlockSpec((block, outputs), lambda i, info: (i, 0)),
            scratch_shapes=[pltpu.VMEM((blocks, each, 3 * cols), F32)],
        ),
        out_shape=jax.ShapeDtypeStruct((own_rows, outputs), BF16),
        compiler_params=limit(24),
        name="project",
    )(
        info,
        off_chip(values),
        *[off_chip(moved[d]) for d in range(1, blocks)],
        *[held(known[d]) for d in range(blocks)],
        held(weight),
    )


def solution(mesh):
    return jax.shard_map(
        on_device,
        mesh=mesh,
        in_specs=(P("shuf", "rep"), P("shuf"), P("shuf", None), P("rep"), P("rep"), P("rep", None)),
        out_specs=P(("shuf", "rep"), None),
        check_vma=False,
    )
```

```python
import jax
import jax.numpy as jnp
from jax import lax
from jax.experimental import pallas as pl
from jax.experimental.pallas import tpu as pltpu
from jax.sharding import PartitionSpec as P


GRP_DEV = 32
PRIOR = 256.0
LANES = 128
MSG = 16
F32 = jnp.float32
BF16 = jnp.bfloat16
MIB = 1 << 20


def iota(shape, dim):
    return lax.broadcasted_iota(jnp.int32, shape, dim)


def exact_dot(one_hot, rows):
    return jnp.dot(one_hot.astype(BF16), rows.astype(BF16), preferred_element_type=F32)


def as_column(row, size, at):
    picked = jnp.where(at == iota((size, size), 1), jnp.broadcast_to(row, (size, size)), 0.0)
    return jnp.sum(picked, axis=1, keepdims=True)


def places(owner_row):
    size = owner_row.shape[1]
    column = as_column(owner_row, size, iota((size, size), 0))
    same = column == jnp.broadcast_to(owner_row, (size, size))
    earlier = iota((size, size), 0) < iota((size, size), 1)
    return jnp.sum(jnp.where(same & earlier, 1.0, 0.0), axis=0, keepdims=True)


def put(scratch, part, peers, at):
    for n in range(part.shape[1] // LANES):
        scratch[pl.ds(at + n, peers, stride=MSG), :] = part[:, n * LANES : (n + 1) * LANES]


def take(scratch, peers, at, count):
    return jnp.concatenate([scratch[pl.ds(at + n, peers, stride=MSG), :] for n in range(count)], axis=1)


def run(copies):
    for copy in copies:
        copy.start()
    for copy in copies:
        copy.wait()


def cut_kernel(values, weight, out, sems, *, rows, blocks):
    half, cols = weight.shape[0] // 2, values.shape[1]
    first = pl.multiple_of(lax.rem(lax.axis_index("rep") + 2, blocks) * rows, rows)
    mine = pl.multiple_of(lax.rem(lax.axis_index("shuf"), 2) * half, half)
    copies = [
        pltpu.make_async_copy(values.at[pl.ds(first, rows), :], out.at[pl.ds(blocks * half, rows), :], sems.at[blocks])
    ]
    for n in range(blocks):
        source = weight.at[pl.ds(mine, half), pl.ds(n * cols, cols)]
        copies.append(pltpu.make_async_copy(source, out.at[pl.ds(n * half, half), :], sems.at[n]))
    run(copies)


def stack_kernel(*refs):
    parts, out = refs[:-1], refs[-1]
    rows, cols = parts[0].shape
    count = out.shape[1] // cols
    half = rows // count
    for n, part in enumerate(parts):
        for c in range(count):
            out[n * half : (n + 1) * half, c * cols : (c + 1) * cols] = part[c * half : (c + 1) * half, :]


def assemble_kernel(near, far, out, sems, *, blocks, cols):
    half = near.shape[0] // blocks
    core = lax.rem(lax.axis_index("shuf"), 2)

    def rows_of(n, number):
        return out.at[pl.ds(pl.multiple_of(n * cols + number * half, half), half), :]

    copies = [
        pltpu.make_async_copy(near.at[pl.ds(n * half, half), :], rows_of(n, core), sems.at[n]) for n in range(blocks)
    ]
    for copy in copies:
        copy.start()
    for n in range(blocks):
        rows_of(n, 1 - core)[...] = far[n * half : (n + 1) * half, :]
    for copy in copies:
        copy.wait()


def quarter_of(step, blocks):
    rank = lax.axis_index("rep")
    return lax.rem(rank + jnp.where(step == 0, 1, jnp.where(step == 1, 3, jnp.where(step == 2, 0, 2))), blocks)


def stats_kernel(values, weight, owner, sub, out, *refs, tiles, peers):
    sent, (first, second, scratch, sems) = refs[:4], refs[4:]
    step = pl.program_id(0)
    rows, cols = values.shape
    blocks = 4
    half, part = weight.shape[0], rows // 2
    here = tiles // blocks
    quarter = quarter_of(step, blocks)

    def copies(n):
        early, late = sent[2 * n : 2 * n + 2]
        for c in range(blocks):
            source = weight.at[:, pl.ds(c * cols, cols)]
            yield pltpu.make_async_copy(source, early.at[pl.ds(c * half, half), :], sems.at[n, c])
        source = values.at[pl.ds(0, part), :]
        yield pltpu.make_async_copy(source, early.at[pl.ds(blocks * half, part), :], sems.at[n, blocks])
        yield pltpu.make_async_copy(values.at[pl.ds(part, part), :], late, sems.at[n, blocks + 1])

    for n in range(2):

        @pl.when(step == n)
        def _():
            for copy in copies(n):
                copy.start()

    tile_rows = rows // here
    chunk = 16

    def one_tile(t, carry):
        low = high = None
        for n in range(tile_rows // chunk):
            at = pl.multiple_of(t * tile_rows + n * chunk, chunk)
            wide = values[pl.ds(at, chunk), :].astype(F32)
            low, high = (wide, wide * wide) if low is None else (low + wide, high + wide * wide)
        at = pl.multiple_of((quarter * here + t) * 8, 8)
        for n in range(cols // LANES):
            lanes = slice(n * LANES, (n + 1) * LANES)
            first[n, pl.ds(at, 8), :] = low[:8, lanes] + low[8:, lanes]
            second[n, pl.ds(at, 8), :] = high[:8, lanes] + high[8:, lanes]
        return carry

    lax.fori_loop(0, here, one_tile, 0, unroll=2)
    for n in range(2):

        @pl.when(step == n)
        def _():
            for copy in copies(n):
                copy.wait()

    @pl.when(step == pl.num_programs(0) - 1)
    def _():
        def folded(ref):
            halves = []
            for n in range(cols // LANES):
                rows = [ref[n, pl.ds(r, tiles, stride=8), :] for r in range(8)]
                while len(rows) > 1:
                    rows = [a + b for a, b in zip(rows[::2], rows[1::2])]
                halves.append(rows[0])
            return jnp.concatenate(halves, axis=1) * (1.0 / tile_rows)

        all_mean = folded(first)
        all_var = folded(second) - all_mean * all_mean
        dev_mean = jnp.sum(all_mean, axis=0, keepdims=True) * (1.0 / tiles)
        apart = all_mean - dev_mean
        dev_var = jnp.sum(all_var + apart * apart, axis=0, keepdims=True) * (1.0 / tiles)
        owner_row = owner[...].astype(F32)
        place = places(owner_row)
        named = jnp.broadcast_to(owner_row, (peers, tiles)) == iota((peers, tiles), 0).astype(F32)
        sub_column = as_column(sub[...].astype(F32), tiles, iota((tiles, tiles), 0))
        sub_wide = jnp.broadcast_to(sub_column + 1.0, (tiles, LANES))
        hot = jnp.concatenate([jnp.where(named & (place == float(slot)), 1.0, 0.0) for slot in range(2)], axis=0)
        sent = exact_dot(hot, jnp.concatenate([all_mean, all_var, sub_wide], axis=1))
        for slot in range(2):
            here = sent[slot * peers : (slot + 1) * peers, :]
            put(scratch, here[:, : 2 * cols], peers, 4 * slot)
            put(scratch, here[:, 2 * cols :] - 1.0, peers, 14 + slot)
        high = dev_mean.astype(BF16).astype(F32)
        put(scratch, jnp.broadcast_to(high, (peers, cols)), peers, 8)
        put(scratch, jnp.broadcast_to(dev_mean - high, (peers, cols)), peers, 10)
        put(scratch, jnp.broadcast_to(dev_var, (peers, cols)), peers, 12)
        out[...] = scratch[...].astype(BF16)


def pair_kernel(gain, bias, out):
    out[0:1, :] = gain[...]
    out[1:2, :] = bias[...]


def owner_kernel(arrived, both, out, scratch, *, peers, tile_rows):
    scratch[...] = arrived[...].astype(F32)
    dev_mean = take(scratch, peers, 8, 2) + take(scratch, peers, 10, 2)
    mean_all = jnp.sum(dev_mean, axis=0, keepdims=True) * (1.0 / peers)
    apart = dev_mean - mean_all
    var_all = jnp.sum(take(scratch, peers, 12, 2) + apart * apart, axis=0, keepdims=True) * (1.0 / peers)
    cols = dev_mean.shape[1]
    forth, back, firsts, seconds = [], [], [], []
    for slot in range(2):
        label = take(scratch, peers, 14 + slot, 1)
        back.append(jnp.where(label[:, :GRP_DEV] == iota((peers, GRP_DEV), 1).astype(F32), 1.0, 0.0))
        on_diagonal = iota((peers, peers), 0) == iota((peers, peers), 1)
        row = jnp.sum(jnp.where(on_diagonal, label[:, :peers], 0.0), axis=0, keepdims=True)
        wide = jnp.broadcast_to(row, (GRP_DEV, peers))
        forth.append(jnp.where(wide == iota((GRP_DEV, peers), 0).astype(F32), 1.0, 0.0))
        shifted = take(scratch, peers, 4 * slot, 2) - mean_all
        firsts.append(shifted)
        seconds.append(take(scratch, peers, 4 * slot + 2, 2) + shifted * shifted)
    forth = jnp.concatenate(forth, axis=1)
    count = jnp.sum(forth, axis=1, keepdims=True) * float(tile_rows)
    data = jnp.concatenate([jnp.concatenate(firsts, axis=0), jnp.concatenate(seconds, axis=0)], axis=1)
    high = data.astype(BF16).astype(F32)
    middle = (data - high).astype(BF16).astype(F32)
    parts = exact_dot(forth, jnp.concatenate([high, middle, data - high - middle], axis=1))
    sums = (parts[:, : 2 * cols] + parts[:, 2 * cols : 4 * cols] + parts[:, 4 * cols :]) * float(tile_rows)
    portion = 1.0 / (count + PRIOR)
    center = sums[:, :cols] * portion
    second = (sums[:, cols:] + PRIOR * var_all) * portion
    inverse = lax.rsqrt(second - center * center + 1e-05)
    scale = (inverse * both[0:1, :]).astype(BF16).astype(F32)
    shift = both[1:2, :] - (center + mean_all) * scale
    shift_high = shift.astype(BF16).astype(F32)
    reply = exact_dot(
        jnp.concatenate(back, axis=0), jnp.concatenate([scale, shift_high, shift - shift_high], axis=1)
    )
    for slot in range(2):
        put(scratch, reply[slot * peers : (slot + 1) * peers, :], peers, 6 * slot)
    out[...] = scratch[...].astype(BF16)


def tile_kernel(arrived, owner, *refs, tiles, peers, blocks):
    outs, scratch = refs[:-1], refs[-1]
    scratch[...] = arrived[...].astype(F32)
    owner_row = owner[...].astype(F32)
    at = (iota((tiles, tiles), 0) + lax.axis_index("rep") * (tiles // blocks)) % tiles
    place = as_column(places(owner_row), tiles, at)
    named = as_column(owner_row, tiles, at) == iota((tiles, peers), 1).astype(F32)
    hot = jnp.concatenate([jnp.where(named & (place == float(slot)), 1.0, 0.0) for slot in range(2)], axis=1)
    rows = jnp.concatenate([take(scratch, peers, 6 * slot, 6) for slot in range(2)], axis=0)
    picked = exact_dot(hot, rows)
    each = tiles // blocks
    for n, out in enumerate(outs):
        out[...] = picked[n * each : (n + 1) * each, :].astype(BF16)


def project_kernel(*refs, blocks, tile_rows, tile_at):
    moved, coeffs, weight, (out, wide) = refs[:blocks], refs[blocks : 2 * blocks], refs[2 * blocks], refs[-2:]
    step = pl.program_id(0)
    rows, cols = moved[0].shape
    tiles = rows // tile_rows

    @pl.when(step == 0)
    def _():
        for n in range(blocks):
            wide[n] = coeffs[n][...].astype(F32)

    strips = []
    for t in range(tiles):
        parts = []
        for n in range(blocks):
            row = wide[n, pl.ds(tile_at + step * tiles + t, 1), :]
            value = moved[n][t * tile_rows : (t + 1) * tile_rows, :].astype(F32)
            scored = value * row[:, :cols] + (row[:, cols : 2 * cols] + row[:, 2 * cols :])
            parts.append(scored.astype(BF16))
        strips.append(jnp.concatenate(parts, axis=1))
    out[...] = jnp.dot(jnp.concatenate(strips, axis=0), weight[...], preferred_element_type=F32).astype(BF16)


def hop(value, axis, distance):
    size = lax.axis_size(axis)
    return lax.ppermute(value, axis, [(i, (i + distance) % size) for i in range(size)])


def whole(*shape):
    return pl.BlockSpec(shape, lambda *_: (0,) * len(shape))


IN_VMEM = pl.BlockSpec(memory_space=pltpu.VMEM)
IN_SMEM = pl.BlockSpec(memory_space=pltpu.SMEM)
IN_HBM = pl.BlockSpec(memory_space=pltpu.HBM)


def limit(mib):
    return pltpu.CompilerParams(vmem_limit_bytes=mib * MIB)


def held(value):
    return pltpu.with_memory_space_constraint(value, pltpu.VMEM)


def off_chip(value):
    return pltpu.with_memory_space_constraint(value, pltpu.HBM)


IN_ANY = pl.BlockSpec(memory_space=pl.ANY)


def on_device(values, subgroup, owners, col_gain, col_bias, out_weight):
    rows, cols = values.shape
    tiles = subgroup.shape[0]
    tile_rows = rows // tiles
    peers, blocks = lax.axis_size("shuf"), lax.axis_size("rep")
    own_rows = rows // blocks
    outputs = out_weight.shape[1]
    owner_row, sub_row = owners.reshape(1, tiles), subgroup.reshape(1, tiles)

    moved = {}
    two = pl.pallas_call(
        lambda *refs: cut_kernel(*refs, rows=own_rows, blocks=blocks),
        in_specs=[IN_HBM, IN_HBM],
        out_specs=IN_VMEM,
        out_shape=pltpu.VMEM((2 * cols + own_rows, cols), BF16),
        scratch_shapes=[pltpu.SemaphoreType.DMA((blocks + 1,))],
        compiler_params=limit(2),
        name="cut",
    )(off_chip(values), off_chip(out_weight))
    moved[2] = hop(two, "rep", 2)

    part = own_rows // 2
    outgoing, one, one_late, three, three_late = pl.pallas_call(
        lambda *refs: stats_kernel(*refs, tiles=tiles, peers=peers),
        grid=(blocks,),
        in_specs=[
            pl.BlockSpec((own_rows, cols), lambda i: (quarter_of(i, blocks), 0)),
            pl.BlockSpec((cols // 2, outputs), lambda i: (lax.rem(lax.axis_index("shuf"), 2), 0)),
            whole(1, tiles),
            whole(1, tiles),
        ],
        out_specs=[whole(peers * MSG, LANES)] + [IN_HBM] * 4,
        scratch_shapes=[
            pltpu.VMEM((cols // LANES, tiles * 8, LANES), F32),
            pltpu.VMEM((cols // LANES, tiles * 8, LANES), F32),
            pltpu.VMEM((peers * MSG, LANES), F32),
            pltpu.SemaphoreType.DMA((2, blocks + 2)),
        ],
        out_shape=[pltpu.HBM((peers * MSG, LANES), BF16)]
        + [pltpu.HBM((2 * cols + part, cols), BF16), pltpu.HBM((part, cols), BF16)] * 2,
        compiler_params=limit(8),
        name="stats",
    )(off_chip(values), off_chip(out_weight), owner_row, sub_row)

    def exchange(message):
        arrived = lax.all_to_all(message.reshape(peers, MSG, LANES), "shuf", 0, 0, tiled=True)
        return held(arrived.reshape(peers * MSG, LANES))

    arrived = exchange(outgoing)

    late = {}
    for d, early_rows in ((1, one), (3, three)):
        moved[d] = hop(early_rows, "rep", d)
    for d, late_rows in ((1, one_late), (3, three_late)):
        late[d] = hop(late_rows, "rep", d)

    both = pl.pallas_call(
        pair_kernel,
        out_shape=jax.ShapeDtypeStruct((2, cols), F32),
        compiler_params=limit(1),
        name="pair",
    )(col_gain.reshape(1, cols), col_bias.reshape(1, cols))
    answer = pl.pallas_call(
        lambda *refs: owner_kernel(*refs, peers=peers, tile_rows=tile_rows),
        in_specs=[IN_VMEM, whole(2, cols)],
        out_shape=pltpu.HBM((peers * MSG, LANES), BF16),
        scratch_shapes=[pltpu.VMEM((peers * MSG, LANES), F32)],
        compiler_params=limit(6),
        name="moments",
    )(arrived, both)
    returned = exchange(answer)

    near = pl.pallas_call(
        stack_kernel,
        grid=(1,),
        in_specs=[whole(2 * cols, cols)] * blocks,
        out_specs=whole(blocks * cols // 2, outputs),
        out_shape=pltpu.HBM((blocks * cols // 2, outputs), BF16),
        compiler_params=limit(8),
        name="stack",
    )(two, moved[1], moved[2], moved[3])
    far = lax.ppermute(near, "shuf", [(i, i ^ 1) for i in range(peers)])
    weight = pl.pallas_call(
        lambda *refs: assemble_kernel(*refs, blocks=blocks, cols=cols),
        in_specs=[IN_HBM, IN_VMEM],
        out_specs=IN_VMEM,
        out_shape=pltpu.VMEM((blocks * cols, outputs), BF16),
        scratch_shapes=[pltpu.SemaphoreType.DMA((blocks,))],
        compiler_params=limit(2),
        name="assemble",
    )(off_chip(near), held(far))

    each = tiles // blocks
    coeffs = pl.pallas_call(
        lambda *refs: tile_kernel(*refs, tiles=tiles, peers=peers, blocks=blocks),
        in_specs=[IN_VMEM, whole(1, tiles)],
        out_specs=[IN_VMEM] * blocks,
        out_shape=[pltpu.VMEM((each, 3 * cols), BF16)] * blocks,
        scratch_shapes=[pltpu.VMEM((peers * MSG, LANES), F32)],
        compiler_params=limit(4),
        name="pick",
    )(returned, owner_row)
    known = {0: coeffs[0]}
    for d in (2, 1, 3):
        known[d] = hop(coeffs[d], "rep", d)

    block = min(256, part)
    steps = part // block
    skipped = 2 * cols // block
    result = []
    for n in range(2):
        at = n * steps
        messages = [(moved[1], skipped), (moved[2], skipped), (moved[3], skipped)]
        if n == 1:
            messages = [(late[1], 0), (moved[2], skipped + at), (late[3], 0)]
        result = [
            pl.pallas_call(
                lambda *refs: project_kernel(
                    *refs, blocks=blocks, tile_rows=tile_rows, tile_at=at * block // tile_rows
                ),
                grid=(steps,),
                in_specs=[
                    pl.BlockSpec((block, cols), lambda i: (lax.axis_index("rep") * (2 * steps) + at + i, 0))
                ]
                + [pl.BlockSpec((block, cols), lambda i, first=first: (first + i, 0)) for _, first in messages]
                + [IN_VMEM] * (blocks + 1)
                + [IN_HBM] * n,
                out_specs=pl.BlockSpec((block, outputs), lambda i: (at + i, 0)),
                scratch_shapes=[pltpu.VMEM((blocks, each, 3 * cols), F32)],
                out_shape=jax.ShapeDtypeStruct((own_rows, outputs), BF16),
                input_output_aliases={2 * blocks + 1: 0} if n else {},
                compiler_params=limit(24),
            )(
                off_chip(values),
                *[off_chip(message) if message is late[1] or message is late[3] else message for message, _ in messages],
                *[held(known[d]) for d in range(blocks)],
                held(weight),
                *[off_chip(array) for array in result],
            )
        ]
    return result[0]


def solution(mesh):
    return jax.shard_map(
        on_device,
        mesh=mesh,
        in_specs=(P("shuf", "rep"), P("shuf"), P("shuf", None), P("rep"), P("rep"), P("rep", None)),
        out_specs=P(("shuf", "rep"), None),
        check_vma=False,
    )
```

```python
import jax
import jax.numpy as jnp
from jax import lax
from jax.experimental import pallas as pl
from jax.experimental.pallas import tpu as pltpu
from jax.sharding import PartitionSpec as P


GRP_DEV = 32
PRIOR = 256.0
LANES = 128
MSG = 16
F32 = jnp.float32
BF16 = jnp.bfloat16
MIB = 1 << 20


def iota(shape, dim):
    return lax.broadcasted_iota(jnp.int32, shape, dim)


def exact_dot(one_hot, rows):
    return jnp.dot(one_hot.astype(BF16), rows.astype(BF16), preferred_element_type=F32)


def as_column(row, size, at):
    picked = jnp.where(at == iota((size, size), 1), jnp.broadcast_to(row, (size, size)), 0.0)
    return jnp.sum(picked, axis=1, keepdims=True)


def places(owner_row):
    size = owner_row.shape[1]
    column = as_column(owner_row, size, iota((size, size), 0))
    same = column == jnp.broadcast_to(owner_row, (size, size))
    earlier = iota((size, size), 0) < iota((size, size), 1)
    return jnp.sum(jnp.where(same & earlier, 1.0, 0.0), axis=0, keepdims=True)


def put(scratch, part, peers, at):
    for n in range(part.shape[1] // LANES):
        scratch[pl.ds(at + n, peers, stride=MSG), :] = part[:, n * LANES : (n + 1) * LANES]


def take(scratch, peers, at, count):
    return jnp.concatenate([scratch[pl.ds(at + n, peers, stride=MSG), :] for n in range(count)], axis=1)


def run(copies):
    for copy in copies:
        copy.start()
    for copy in copies:
        copy.wait()


def slab_of(depth, slabs):
    index = lax.axis_index("shuf")
    return lax.rem(index // (2 * depth), slabs // 2) * 2 + lax.rem(index, 2)


def cut_kernel(values, weight, out, out_slab, sems, *, rows, blocks, depth):
    slab, cols = out_slab.shape[0], values.shape[1]
    first = pl.multiple_of(lax.rem(lax.axis_index("rep") + 2, blocks) * rows, rows)
    mine = pl.multiple_of(slab_of(depth, weight.shape[0] // slab) * slab, slab)
    copies = [
        pltpu.make_async_copy(values.at[pl.ds(first, rows), :], out.at[pl.ds(blocks * slab, rows), :], sems.at[blocks]),
        pltpu.make_async_copy(weight.at[pl.ds(mine, slab), :], out_slab, sems.at[blocks + 1]),
    ]
    for n in range(blocks):
        source = weight.at[pl.ds(mine, slab), pl.ds(n * cols, cols)]
        copies.append(pltpu.make_async_copy(source, out.at[pl.ds(n * slab, slab), :], sems.at[n]))
    run(copies)


def stack_kernel(own, one, two, three, out):
    slab, cols = own.shape[0], two.shape[1]
    for n, part in ((0, own), (1, one), (3, three)):
        out[n * slab : (n + 1) * slab, :] = part[...]
    for c in range(own.shape[1] // cols):
        out[2 * slab : 3 * slab, c * cols : (c + 1) * cols] = two[c * slab : (c + 1) * slab, :]


def assemble_kernel(mine, sibling, across, across_sibling, out, *, blocks, cols, depth):
    slab = mine.shape[0] // blocks
    slabs = cols // slab
    first = slab_of(depth, slabs)
    core = lax.rem(first, 2)
    parts = (
        (mine, first),
        (sibling, first + 1 - 2 * core),
        (across, lax.rem(first + 2, slabs)),
        (across_sibling, lax.rem(first + 2, slabs) + 1 - 2 * core),
    )
    for part, number in parts:
        for n in range(blocks):
            at = pl.multiple_of(n * cols + number * slab, slab)
            out[pl.ds(at, slab), :] = part[n * slab : (n + 1) * slab, :]


def stats_kernel(values, two, owner, sub, out, one, three, *scratches, tiles, peers):
    held_rows, first, second, scratch, sems_in, sems_out = scratches
    rows, cols = one.shape
    blocks, pieces = 4, 2
    here, size = tiles // blocks, rows // pieces
    rank = lax.axis_index("rep")
    tile_rows = rows // here
    chunk = 16
    places_of = {1: held_rows.at[0], 3: held_rows.at[1], 0: held_rows.at[2]}

    def inward(d, p):
        at = pl.multiple_of(lax.rem(rank + d, blocks) * rows + p * size, size)
        target = places_of[d].at[pl.ds(p * size, size), :]
        return pltpu.make_async_copy(values.at[pl.ds(at, size), :], target, sems_in.at[d, p])

    for d in (1, 3, 0):
        for p in range(pieces):
            inward(d, p).start()

    def moments_of(source, d, p):
        def one_tile(t, carry):
            low = high = None
            for n in range(tile_rows // chunk):
                at = pl.multiple_of(t * tile_rows + n * chunk, chunk)
                wide = source[pl.ds(at, chunk), :].astype(F32)
                low, high = (wide, wide * wide) if low is None else (low + wide, high + wide * wide)
            tile = lax.rem(rank + d, blocks) * here + p * (here // pieces) + t
            at = pl.multiple_of(tile * 8, 8)
            for n in range(cols // LANES):
                lanes = slice(n * LANES, (n + 1) * LANES)
                first[n, pl.ds(at, 8), :] = low[:8, lanes] + low[8:, lanes]
                second[n, pl.ds(at, 8), :] = high[:8, lanes] + high[8:, lanes]
            return carry

        lax.fori_loop(0, here // pieces, one_tile, 0, unroll=2)

    skipped = two.shape[0] - rows
    for p in range(pieces):
        moments_of(two.at[pl.ds(skipped + p * size, size), :], 2, p)
    outward = []
    for d in (1, 3, 0):
        for p in range(pieces):
            inward(d, p).wait()
            if d and p == pieces - 1:
                outward.append(pltpu.make_async_copy(places_of[d], one if d == 1 else three, sems_out.at[d // 2]))
                outward[-1].start()
            moments_of(places_of[d].at[pl.ds(p * size, size), :], d, p)

    def folded(ref):
        halves = []
        for n in range(cols // LANES):
            summed = [ref[n, pl.ds(r, tiles, stride=8), :] for r in range(8)]
            while len(summed) > 1:
                summed = [a + b for a, b in zip(summed[::2], summed[1::2])]
            halves.append(summed[0])
        return jnp.concatenate(halves, axis=1) * (1.0 / tile_rows)

    all_mean = folded(first)
    all_var = folded(second) - all_mean * all_mean
    dev_mean = jnp.sum(all_mean, axis=0, keepdims=True) * (1.0 / tiles)
    apart = all_mean - dev_mean
    dev_var = jnp.sum(all_var + apart * apart, axis=0, keepdims=True) * (1.0 / tiles)
    owner_row = owner[...].astype(F32)
    place = places(owner_row)
    named = jnp.broadcast_to(owner_row, (peers, tiles)) == iota((peers, tiles), 0).astype(F32)
    sub_column = as_column(sub[...].astype(F32), tiles, iota((tiles, tiles), 0))
    sub_wide = jnp.broadcast_to(sub_column + 1.0, (tiles, LANES))
    hot = jnp.concatenate([jnp.where(named & (place == float(slot)), 1.0, 0.0) for slot in range(2)], axis=0)
    sent = exact_dot(hot, jnp.concatenate([all_mean, all_var, sub_wide], axis=1))
    for slot in range(2):
        message = sent[slot * peers : (slot + 1) * peers, :]
        put(scratch, message[:, : 2 * cols], peers, 4 * slot)
        put(scratch, message[:, 2 * cols :] - 1.0, peers, 14 + slot)
    high = dev_mean.astype(BF16).astype(F32)
    put(scratch, jnp.broadcast_to(high, (peers, cols)), peers, 8)
    put(scratch, jnp.broadcast_to(dev_mean - high, (peers, cols)), peers, 10)
    put(scratch, jnp.broadcast_to(dev_var, (peers, cols)), peers, 12)
    out[...] = scratch[...].astype(BF16)
    for copy in outward:
        copy.wait()


def pair_kernel(gain, bias, out):
    out[0:1, :] = gain[...]
    out[1:2, :] = bias[...]


def owner_kernel(arrived, both, out, scratch, *, peers, tile_rows):
    scratch[...] = arrived[...].astype(F32)
    dev_mean = take(scratch, peers, 8, 2) + take(scratch, peers, 10, 2)
    mean_all = jnp.sum(dev_mean, axis=0, keepdims=True) * (1.0 / peers)
    apart = dev_mean - mean_all
    var_all = jnp.sum(take(scratch, peers, 12, 2) + apart * apart, axis=0, keepdims=True) * (1.0 / peers)
    cols = dev_mean.shape[1]
    forth, back, firsts, seconds = [], [], [], []
    for slot in range(2):
        label = take(scratch, peers, 14 + slot, 1)
        back.append(jnp.where(label[:, :GRP_DEV] == iota((peers, GRP_DEV), 1).astype(F32), 1.0, 0.0))
        on_diagonal = iota((peers, peers), 0) == iota((peers, peers), 1)
        row = jnp.sum(jnp.where(on_diagonal, label[:, :peers], 0.0), axis=0, keepdims=True)
        wide = jnp.broadcast_to(row, (GRP_DEV, peers))
        forth.append(jnp.where(wide == iota((GRP_DEV, peers), 0).astype(F32), 1.0, 0.0))
        shifted = take(scratch, peers, 4 * slot, 2) - mean_all
        firsts.append(shifted)
        seconds.append(take(scratch, peers, 4 * slot + 2, 2) + shifted * shifted)
    forth = jnp.concatenate(forth, axis=1)
    count = jnp.sum(forth, axis=1, keepdims=True) * float(tile_rows)
    data = jnp.concatenate([jnp.concatenate(firsts, axis=0), jnp.concatenate(seconds, axis=0)], axis=1)
    high = data.astype(BF16).astype(F32)
    middle = (data - high).astype(BF16).astype(F32)
    parts = exact_dot(forth, jnp.concatenate([high, middle, data - high - middle], axis=1))
    sums = (parts[:, : 2 * cols] + parts[:, 2 * cols : 4 * cols] + parts[:, 4 * cols :]) * float(tile_rows)
    portion = 1.0 / (count + PRIOR)
    center = sums[:, :cols] * portion
    second = (sums[:, cols:] + PRIOR * var_all) * portion
    inverse = lax.rsqrt(second - center * center + 1e-05)
    scale = (inverse * both[0:1, :]).astype(BF16).astype(F32)
    shift = both[1:2, :] - (center + mean_all) * scale
    shift_high = shift.astype(BF16).astype(F32)
    reply = exact_dot(
        jnp.concatenate(back, axis=0), jnp.concatenate([scale, shift_high, shift - shift_high], axis=1)
    )
    for slot in range(2):
        put(scratch, reply[slot * peers : (slot + 1) * peers, :], peers, 6 * slot)
    out[...] = scratch[...].astype(BF16)


def tile_kernel(arrived, owner, *refs, tiles, peers, blocks):
    outs, scratch = refs[:-1], refs[-1]
    scratch[...] = arrived[...].astype(F32)
    owner_row = owner[...].astype(F32)
    at = (iota((tiles, tiles), 0) + lax.axis_index("rep") * (tiles // blocks)) % tiles
    place = as_column(places(owner_row), tiles, at)
    named = as_column(owner_row, tiles, at) == iota((tiles, peers), 1).astype(F32)
    hot = jnp.concatenate([jnp.where(named & (place == float(slot)), 1.0, 0.0) for slot in range(2)], axis=1)
    rows = jnp.concatenate([take(scratch, peers, 6 * slot, 6) for slot in range(2)], axis=0)
    picked = exact_dot(hot, rows)
    each = tiles // blocks
    for n, out in enumerate(outs):
        out[...] = picked[n * each : (n + 1) * each, :].astype(BF16)


def project_kernel(*refs, blocks, tile_rows, block, skipped):
    moved, coeffs, weight, out = refs[:blocks], refs[blocks : 2 * blocks], refs[2 * blocks], refs[2 * blocks + 1]
    held_rows, result, wide, sems_in, sems_out = refs[-5:]
    _, rows, cols = held_rows.shape
    skipped = (lax.axis_index("rep") * rows, *skipped)
    tiles = block // tile_rows
    steps = rows // block

    def inward(n, j):
        source = moved[n].at[pl.ds(pl.multiple_of(skipped[n] + j * block, block), block), :]
        return pltpu.make_async_copy(source, held_rows.at[n, pl.ds(j * block, block), :], sems_in.at[n, j])

    def outward(j):
        part = pl.ds(j * block, block)
        return pltpu.make_async_copy(result.at[part, :], out.at[part, :], sems_out.at[j])

    for j in range(steps):
        for n in range(blocks):
            inward(n, j).start()
    for n in range(blocks):
        wide[n] = coeffs[n][...].astype(F32)
    for j in range(steps):
        for n in range(blocks):
            inward(n, j).wait()
        strips = []
        for t in range(tiles):
            at = j * block + t * tile_rows
            parts = []
            for n in range(blocks):
                row = wide[n, j * tiles + t : j * tiles + t + 1, :]
                value = held_rows[n, at : at + tile_rows, :]
                scored = value.astype(F32) * row[:, :cols] + (row[:, cols : 2 * cols] + row[:, 2 * cols :])
                parts.append(scored.astype(BF16))
            strips.append(jnp.concatenate(parts, axis=1))
        product = jnp.dot(jnp.concatenate(strips, axis=0), weight[...], preferred_element_type=F32)
        result[j * block : (j + 1) * block, :] = product.astype(BF16)
        outward(j).start()
    for j in range(steps):
        outward(j).wait()


def hop(value, axis, distance):
    size = lax.axis_size(axis)
    return lax.ppermute(value, axis, [(i, (i + distance) % size) for i in range(size)])


def whole(*shape):
    return pl.BlockSpec(shape, lambda *_: (0,) * len(shape))


IN_VMEM = pl.BlockSpec(memory_space=pltpu.VMEM)
IN_SMEM = pl.BlockSpec(memory_space=pltpu.SMEM)
IN_HBM = pl.BlockSpec(memory_space=pltpu.HBM)


def limit(mib):
    return pltpu.CompilerParams(vmem_limit_bytes=mib * MIB)


def held(value):
    return pltpu.with_memory_space_constraint(value, pltpu.VMEM)


def off_chip(value):
    return pltpu.with_memory_space_constraint(value, pltpu.HBM)


IN_ANY = pl.BlockSpec(memory_space=pl.ANY)


def on_device(values, subgroup, owners, col_gain, col_bias, out_weight):
    rows, cols = values.shape
    tiles = subgroup.shape[0]
    tile_rows = rows // tiles
    peers, blocks = lax.axis_size("shuf"), lax.axis_size("rep")
    own_rows = rows // blocks
    outputs = out_weight.shape[1]
    owner_row, sub_row = owners.reshape(1, tiles), subgroup.reshape(1, tiles)

    depth = max(1, peers // 8)
    slab = cols // 4
    moved = {}
    two, own_slab = pl.pallas_call(
        lambda *refs: cut_kernel(*refs, rows=own_rows, blocks=blocks, depth=depth),
        in_specs=[IN_HBM, IN_HBM],
        out_specs=[IN_VMEM] * 2,
        out_shape=[pltpu.VMEM((cols + own_rows, cols), BF16), pltpu.VMEM((slab, outputs), BF16)],
        scratch_shapes=[pltpu.SemaphoreType.DMA((blocks + 2,))],
        compiler_params=limit(2),
        name="cut",
    )(off_chip(values), off_chip(out_weight))
    moved[2] = hop(two, "rep", 2)

    outgoing, one, three = pl.pallas_call(
        lambda *refs: stats_kernel(*refs, tiles=tiles, peers=peers),
        grid=(1,),
        in_specs=[IN_HBM, IN_VMEM, whole(1, tiles), whole(1, tiles)],
        out_specs=[whole(peers * MSG, LANES), IN_HBM, IN_HBM],
        scratch_shapes=[
            pltpu.VMEM((3, own_rows, cols), BF16),
            pltpu.VMEM((cols // LANES, tiles * 8, LANES), F32),
            pltpu.VMEM((cols // LANES, tiles * 8, LANES), F32),
            pltpu.VMEM((peers * MSG, LANES), F32),
            pltpu.SemaphoreType.DMA((blocks, 2)),
            pltpu.SemaphoreType.DMA((2,)),
        ],
        out_shape=[
            pltpu.HBM((peers * MSG, LANES), BF16), pltpu.HBM((own_rows, cols), BF16), pltpu.HBM((own_rows, cols), BF16)
        ],
        compiler_params=limit(8),
        name="stats",
    )(off_chip(values), held(two), owner_row, sub_row)

    def exchange(message):
        arrived = lax.all_to_all(message.reshape(peers, MSG, LANES), "shuf", 0, 0, tiled=True)
        return held(arrived.reshape(peers * MSG, LANES))

    arrived = exchange(outgoing)

    slabs = {0: own_slab}
    for d in (1, 3):
        slabs[d] = hop(own_slab, "rep", d)
    for d, sent in ((1, one), (3, three)):
        moved[d] = hop(sent, "rep", d)

    both = pl.pallas_call(
        pair_kernel,
        out_shape=jax.ShapeDtypeStruct((2, cols), F32),
        compiler_params=limit(1),
        name="pair",
    )(col_gain.reshape(1, cols), col_bias.reshape(1, cols))
    answer = pl.pallas_call(
        lambda *refs: owner_kernel(*refs, peers=peers, tile_rows=tile_rows),
        in_specs=[IN_VMEM, whole(2, cols)],
        out_shape=pltpu.HBM((peers * MSG, LANES), BF16),
        scratch_shapes=[pltpu.VMEM((peers * MSG, LANES), F32)],
        compiler_params=limit(6),
        name="moments",
    )(arrived, both)
    returned = exchange(answer)

    def trade(value, distance):
        return lax.ppermute(value, "shuf", [(i, i ^ distance) for i in range(peers)])

    mine = pl.pallas_call(
        stack_kernel,
        grid=(1,),
        in_specs=[whole(slab, outputs), whole(slab, outputs), whole(cols, cols), whole(slab, outputs)],
        out_specs=whole(cols, outputs),
        out_shape=pltpu.HBM((cols, outputs), BF16),
        compiler_params=limit(8),
        name="stack",
    )(slabs[0], slabs[1], moved[2], slabs[3])
    across = trade(mine, 2 * depth)
    sibling = trade(mine, 1)
    across_sibling = trade(across, 1)
    weight = pl.pallas_call(
        lambda *refs: assemble_kernel(*refs, blocks=blocks, cols=cols, depth=depth),
        grid=(1,),
        in_specs=[whole(cols, outputs)] * 3 + [IN_VMEM],
        out_specs=IN_VMEM,
        out_shape=pltpu.VMEM((blocks * cols, outputs), BF16),
        compiler_params=limit(8),
        name="assemble",
    )(mine, sibling, across, held(across_sibling))

    each = tiles // blocks
    coeffs = pl.pallas_call(
        lambda *refs: tile_kernel(*refs, tiles=tiles, peers=peers, blocks=blocks),
        in_specs=[IN_VMEM, whole(1, tiles)],
        out_specs=[IN_VMEM] * blocks,
        out_shape=[pltpu.VMEM((each, 3 * cols), BF16)] * blocks,
        scratch_shapes=[pltpu.VMEM((peers * MSG, LANES), F32)],
        compiler_params=limit(4),
        name="pick",
    )(returned, owner_row)
    known = {0: coeffs[0]}
    for d in (2, 1, 3):
        known[d] = hop(coeffs[d], "rep", d)

    block = min(256, own_rows)
    return pl.pallas_call(
        lambda *refs: project_kernel(
            *refs, blocks=blocks, tile_rows=tile_rows, block=block, skipped=(0, two.shape[0] - own_rows, 0)
        ),
        in_specs=[IN_HBM] * blocks + [IN_VMEM] * (blocks + 1),
        out_specs=IN_HBM,
        out_shape=pltpu.HBM((own_rows, outputs), BF16),
        scratch_shapes=[
            pltpu.VMEM((blocks, own_rows, cols), BF16),
            pltpu.VMEM((own_rows, outputs), BF16),
            pltpu.VMEM((blocks, each, 3 * cols), F32),
            pltpu.SemaphoreType.DMA((blocks, own_rows // block)),
            pltpu.SemaphoreType.DMA((own_rows // block,)),
        ],
        compiler_params=limit(24),
        name="project",
    )(
        off_chip(values),
        *[off_chip(moved[d]) for d in range(1, blocks)],
        *[held(known[d]) for d in range(blocks)],
        held(weight),
    )


def solution(mesh):
    return jax.shard_map(
        on_device,
        mesh=mesh,
        in_specs=(P("shuf", "rep"), P("shuf"), P("shuf", None), P("rep"), P("rep"), P("rep", None)),
        out_specs=P(("shuf", "rep"), None),
        check_vma=False,
    )
```

```python
import jax
import jax.numpy as jnp
from jax import lax
from jax.experimental import pallas as pl
from jax.experimental.pallas import tpu as pltpu
from jax.sharding import PartitionSpec as P


GRP_DEV = 32
PRIOR = 256.0
LANES = 128
MSG = 16
F32 = jnp.float32
BF16 = jnp.bfloat16
MIB = 1 << 20


def iota(shape, dim):
    return lax.broadcasted_iota(jnp.int32, shape, dim)


def exact_dot(one_hot, rows):
    return jnp.dot(one_hot.astype(BF16), rows.astype(BF16), preferred_element_type=F32)


def as_column(row, size, at):
    picked = jnp.where(at == iota((size, size), 1), jnp.broadcast_to(row, (size, size)), 0.0)
    return jnp.sum(picked, axis=1, keepdims=True)


def places(owner_row):
    size = owner_row.shape[1]
    column = as_column(owner_row, size, iota((size, size), 0))
    same = column == jnp.broadcast_to(owner_row, (size, size))
    earlier = iota((size, size), 0) < iota((size, size), 1)
    return jnp.sum(jnp.where(same & earlier, 1.0, 0.0), axis=0, keepdims=True)


def put(scratch, part, peers, at):
    for n in range(part.shape[1] // LANES):
        scratch[pl.ds(at + n, peers, stride=MSG), :] = part[:, n * LANES : (n + 1) * LANES]


def take(scratch, peers, at, count):
    return jnp.concatenate([scratch[pl.ds(at + n, peers, stride=MSG), :] for n in range(count)], axis=1)


def run(copies):
    for copy in copies:
        copy.start()
    for copy in copies:
        copy.wait()


def slab_of(depth, slabs):
    index = lax.axis_index("shuf")
    return lax.rem(index // (2 * depth), slabs // 2) * 2 + lax.rem(index, 2)


def cut_kernel(values, weight, out, out_slab, sems, *, rows, blocks, depth):
    slab, cols = out_slab.shape[0], values.shape[1]
    first = pl.multiple_of(lax.rem(lax.axis_index("rep") + 2, blocks) * rows, rows)
    mine = pl.multiple_of(slab_of(depth, weight.shape[0] // slab) * slab, slab)
    copies = [
        pltpu.make_async_copy(values.at[pl.ds(first, rows), :], out.at[pl.ds(blocks * slab, rows), :], sems.at[blocks]),
        pltpu.make_async_copy(weight.at[pl.ds(mine, slab), :], out_slab, sems.at[blocks + 1]),
    ]
    for n in range(blocks):
        source = weight.at[pl.ds(mine, slab), pl.ds(n * cols, cols)]
        copies.append(pltpu.make_async_copy(source, out.at[pl.ds(n * slab, slab), :], sems.at[n]))
    run(copies)


def stack_kernel(own, one, two, three, out):
    slab, cols = own.shape[0], two.shape[1]
    for n, part in ((0, own), (1, one), (3, three)):
        out[n * slab : (n + 1) * slab, :] = part[...]
    for c in range(own.shape[1] // cols):
        out[2 * slab : 3 * slab, c * cols : (c + 1) * cols] = two[c * slab : (c + 1) * slab, :]


def assemble_kernel(mine, sibling, across, across_sibling, out, *, blocks, cols, depth):
    slab = mine.shape[0] // blocks
    slabs = cols // slab
    first = slab_of(depth, slabs)
    core = lax.rem(first, 2)
    parts = (
        (mine, first),
        (sibling, first + 1 - 2 * core),
        (across, lax.rem(first + 2, slabs)),
        (across_sibling, lax.rem(first + 2, slabs) + 1 - 2 * core),
    )
    for part, number in parts:
        for n in range(blocks):
            at = pl.multiple_of(n * cols + number * slab, slab)
            out[pl.ds(at, slab), :] = part[n * slab : (n + 1) * slab, :]


def stats_kernel(values, two, owner, sub, out, one, three, *scratches, tiles, peers):
    held_rows, first, second, scratch, sems_in, sems_out = scratches
    rows, cols = one.shape
    blocks, pieces = 4, 2
    here, size = tiles // blocks, rows // pieces
    rank = lax.axis_index("rep")
    tile_rows = rows // here
    chunk = 16
    places_of = {1: held_rows.at[0], 3: held_rows.at[1], 0: held_rows.at[2]}

    def inward(d, p):
        at = pl.multiple_of(lax.rem(rank + d, blocks) * rows + p * size, size)
        target = places_of[d].at[pl.ds(p * size, size), :]
        return pltpu.make_async_copy(values.at[pl.ds(at, size), :], target, sems_in.at[d, p])

    for d in (1, 3, 0):
        for p in range(pieces):
            inward(d, p).start()

    def moments_of(source, d, p):
        def one_tile(t, carry):
            low = high = None
            for n in range(tile_rows // chunk):
                at = pl.multiple_of(t * tile_rows + n * chunk, chunk)
                wide = source[pl.ds(at, chunk), :].astype(F32)
                low, high = (wide, wide * wide) if low is None else (low + wide, high + wide * wide)
            tile = lax.rem(rank + d, blocks) * here + p * (here // pieces) + t
            at = pl.multiple_of(tile * 8, 8)
            for n in range(cols // LANES):
                lanes = slice(n * LANES, (n + 1) * LANES)
                first[n, pl.ds(at, 8), :] = low[:8, lanes] + low[8:, lanes]
                second[n, pl.ds(at, 8), :] = high[:8, lanes] + high[8:, lanes]
            return carry

        lax.fori_loop(0, here // pieces, one_tile, 0, unroll=2)

    skipped = two.shape[0] - rows
    for p in range(pieces):
        moments_of(two.at[pl.ds(skipped + p * size, size), :], 2, p)
    outward = []
    for d in (1, 3, 0):
        for p in range(pieces):
            inward(d, p).wait()
            if d and p == pieces - 1:
                outward.append(pltpu.make_async_copy(places_of[d], one if d == 1 else three, sems_out.at[d // 2]))
                outward[-1].start()
            moments_of(places_of[d].at[pl.ds(p * size, size), :], d, p)

    def folded(ref):
        halves = []
        for n in range(cols // LANES):
            summed = [ref[n, pl.ds(r, tiles, stride=8), :] for r in range(8)]
            while len(summed) > 1:
                summed = [a + b for a, b in zip(summed[::2], summed[1::2])]
            halves.append(summed[0])
        return jnp.concatenate(halves, axis=1) * (1.0 / tile_rows)

    all_mean = folded(first)
    all_var = folded(second) - all_mean * all_mean
    dev_mean = jnp.sum(all_mean, axis=0, keepdims=True) * (1.0 / tiles)
    apart = all_mean - dev_mean
    dev_var = jnp.sum(all_var + apart * apart, axis=0, keepdims=True) * (1.0 / tiles)
    owner_row = owner[...].astype(F32)
    place = places(owner_row)
    named = jnp.broadcast_to(owner_row, (peers, tiles)) == iota((peers, tiles), 0).astype(F32)
    sub_column = as_column(sub[...].astype(F32), tiles, iota((tiles, tiles), 0))
    sub_wide = jnp.broadcast_to(sub_column + 1.0, (tiles, LANES))
    hot = jnp.concatenate([jnp.where(named & (place == float(slot)), 1.0, 0.0) for slot in range(2)], axis=0)
    sent = exact_dot(hot, jnp.concatenate([all_mean, all_var, sub_wide], axis=1))
    for slot in range(2):
        message = sent[slot * peers : (slot + 1) * peers, :]
        put(scratch, message[:, : 2 * cols], peers, 4 * slot)
        put(scratch, message[:, 2 * cols :] - 1.0, peers, 14 + slot)
    high = dev_mean.astype(BF16).astype(F32)
    put(scratch, jnp.broadcast_to(high, (peers, cols)), peers, 8)
    put(scratch, jnp.broadcast_to(dev_mean - high, (peers, cols)), peers, 10)
    put(scratch, jnp.broadcast_to(dev_var, (peers, cols)), peers, 12)
    out[...] = scratch[...].astype(BF16)
    for copy in outward:
        copy.wait()


def pair_kernel(gain, bias, out):
    out[0:1, :] = gain[...]
    out[1:2, :] = bias[...]


def owner_kernel(arrived, both, out, scratch, *, peers, tile_rows):
    scratch[...] = arrived[...].astype(F32)
    dev_mean = take(scratch, peers, 8, 2) + take(scratch, peers, 10, 2)
    mean_all = jnp.sum(dev_mean, axis=0, keepdims=True) * (1.0 / peers)
    apart = dev_mean - mean_all
    var_all = jnp.sum(take(scratch, peers, 12, 2) + apart * apart, axis=0, keepdims=True) * (1.0 / peers)
    cols = dev_mean.shape[1]
    forth, back, firsts, seconds = [], [], [], []
    for slot in range(2):
        label = take(scratch, peers, 14 + slot, 1)
        back.append(jnp.where(label[:, :GRP_DEV] == iota((peers, GRP_DEV), 1).astype(F32), 1.0, 0.0))
        on_diagonal = iota((peers, peers), 0) == iota((peers, peers), 1)
        row = jnp.sum(jnp.where(on_diagonal, label[:, :peers], 0.0), axis=0, keepdims=True)
        wide = jnp.broadcast_to(row, (GRP_DEV, peers))
        forth.append(jnp.where(wide == iota((GRP_DEV, peers), 0).astype(F32), 1.0, 0.0))
        shifted = take(scratch, peers, 4 * slot, 2) - mean_all
        firsts.append(shifted)
        seconds.append(take(scratch, peers, 4 * slot + 2, 2) + shifted * shifted)
    forth = jnp.concatenate(forth, axis=1)
    count = jnp.sum(forth, axis=1, keepdims=True) * float(tile_rows)
    data = jnp.concatenate([jnp.concatenate(firsts, axis=0), jnp.concatenate(seconds, axis=0)], axis=1)
    high = data.astype(BF16).astype(F32)
    middle = (data - high).astype(BF16).astype(F32)
    parts = exact_dot(forth, jnp.concatenate([high, middle, data - high - middle], axis=1))
    sums = (parts[:, : 2 * cols] + parts[:, 2 * cols : 4 * cols] + parts[:, 4 * cols :]) * float(tile_rows)
    portion = 1.0 / (count + PRIOR)
    center = sums[:, :cols] * portion
    second = (sums[:, cols:] + PRIOR * var_all) * portion
    inverse = lax.rsqrt(second - center * center + 1e-05)
    scale = (inverse * both[0:1, :]).astype(BF16).astype(F32)
    shift = both[1:2, :] - (center + mean_all) * scale
    shift_high = shift.astype(BF16).astype(F32)
    reply = exact_dot(
        jnp.concatenate(back, axis=0), jnp.concatenate([scale, shift_high, shift - shift_high], axis=1)
    )
    for slot in range(2):
        put(scratch, reply[slot * peers : (slot + 1) * peers, :], peers, 6 * slot)
    out[...] = scratch[...].astype(BF16)


def tile_kernel(arrived, owner, *refs, tiles, peers, blocks):
    outs, scratch = refs[:-1], refs[-1]
    scratch[...] = arrived[...].astype(F32)
    owner_row = owner[...].astype(F32)
    at = (iota((tiles, tiles), 0) + lax.axis_index("rep") * (tiles // blocks)) % tiles
    place = as_column(places(owner_row), tiles, at)
    named = as_column(owner_row, tiles, at) == iota((tiles, peers), 1).astype(F32)
    hot = jnp.concatenate([jnp.where(named & (place == float(slot)), 1.0, 0.0) for slot in range(2)], axis=1)
    rows = jnp.concatenate([take(scratch, peers, 6 * slot, 6) for slot in range(2)], axis=0)
    picked = exact_dot(hot, rows)
    each = tiles // blocks
    for n, out in enumerate(outs):
        out[...] = picked[n * each : (n + 1) * each, :].astype(BF16)


def project_kernel(*refs, blocks, tile_rows, block, skipped):
    moved, coeffs, weight, out = refs[:blocks], refs[blocks : 2 * blocks], refs[2 * blocks], refs[2 * blocks + 1]
    held_rows, result, wide, sems_in, sems_out = refs[-5:]
    _, rows, cols = held_rows.shape
    skipped = (lax.axis_index("rep") * rows, *skipped)
    parts = ((0, block), (block, rows - block)) if rows > block else ((0, rows),)
    tiles = block // tile_rows
    steps = rows // block

    def inward(n, p):
        at, size = parts[p]
        source = moved[n].at[pl.ds(pl.multiple_of(skipped[n] + at, tile_rows), size), :]
        return pltpu.make_async_copy(source, held_rows.at[n, pl.ds(at, size), :], sems_in.at[n, p])

    def outward(j):
        part = pl.ds(j * block, block)
        return pltpu.make_async_copy(result.at[part, :], out.at[part, :], sems_out.at[j])

    for p in range(len(parts)):
        for n in range(blocks):
            inward(n, p).start()
    for n in range(blocks):
        wide[n] = coeffs[n][...].astype(F32)
    for j in range(steps):
        if j < len(parts):
            for n in range(blocks):
                inward(n, j).wait()
        strips = []
        for t in range(tiles):
            at = j * block + t * tile_rows
            scores = []
            for n in range(blocks):
                row = wide[n, j * tiles + t : j * tiles + t + 1, :]
                value = held_rows[n, at : at + tile_rows, :]
                scored = value.astype(F32) * row[:, :cols] + (row[:, cols : 2 * cols] + row[:, 2 * cols :])
                scores.append(scored.astype(BF16))
            strips.append(jnp.concatenate(scores, axis=1))
        product = jnp.dot(jnp.concatenate(strips, axis=0), weight[...], preferred_element_type=F32)
        result[j * block : (j + 1) * block, :] = product.astype(BF16)
        outward(j).start()
    for j in range(steps):
        outward(j).wait()


def hop(value, axis, distance):
    size = lax.axis_size(axis)
    return lax.ppermute(value, axis, [(i, (i + distance) % size) for i in range(size)])


def whole(*shape):
    return pl.BlockSpec(shape, lambda *_: (0,) * len(shape))


IN_VMEM = pl.BlockSpec(memory_space=pltpu.VMEM)
IN_SMEM = pl.BlockSpec(memory_space=pltpu.SMEM)
IN_HBM = pl.BlockSpec(memory_space=pltpu.HBM)


def limit(mib):
    return pltpu.CompilerParams(vmem_limit_bytes=mib * MIB)


def held(value):
    return pltpu.with_memory_space_constraint(value, pltpu.VMEM)


def off_chip(value):
    return pltpu.with_memory_space_constraint(value, pltpu.HBM)


IN_ANY = pl.BlockSpec(memory_space=pl.ANY)


def on_device(values, subgroup, owners, col_gain, col_bias, out_weight):
    rows, cols = values.shape
    tiles = subgroup.shape[0]
    tile_rows = rows // tiles
    peers, blocks = lax.axis_size("shuf"), lax.axis_size("rep")
    own_rows = rows // blocks
    outputs = out_weight.shape[1]
    owner_row, sub_row = owners.reshape(1, tiles), subgroup.reshape(1, tiles)

    depth = max(1, peers // 8)
    slab = cols // 4
    moved = {}
    two, own_slab = pl.pallas_call(
        lambda *refs: cut_kernel(*refs, rows=own_rows, blocks=blocks, depth=depth),
        in_specs=[IN_HBM, IN_HBM],
        out_specs=[IN_VMEM] * 2,
        out_shape=[pltpu.VMEM((cols + own_rows, cols), BF16), pltpu.VMEM((slab, outputs), BF16)],
        scratch_shapes=[pltpu.SemaphoreType.DMA((blocks + 2,))],
        compiler_params=limit(2),
        name="cut",
    )(off_chip(values), off_chip(out_weight))
    moved[2] = hop(two, "rep", 2)

    outgoing, one, three = pl.pallas_call(
        lambda *refs: stats_kernel(*refs, tiles=tiles, peers=peers),
        grid=(1,),
        in_specs=[IN_HBM, IN_VMEM, whole(1, tiles), whole(1, tiles)],
        out_specs=[whole(peers * MSG, LANES), IN_HBM, IN_HBM],
        scratch_shapes=[
            pltpu.VMEM((3, own_rows, cols), BF16),
            pltpu.VMEM((cols // LANES, tiles * 8, LANES), F32),
            pltpu.VMEM((cols // LANES, tiles * 8, LANES), F32),
            pltpu.VMEM((peers * MSG, LANES), F32),
            pltpu.SemaphoreType.DMA((blocks, 2)),
            pltpu.SemaphoreType.DMA((2,)),
        ],
        out_shape=[
            pltpu.HBM((peers * MSG, LANES), BF16), pltpu.HBM((own_rows, cols), BF16), pltpu.HBM((own_rows, cols), BF16)
        ],
        compiler_params=limit(8),
        name="stats",
    )(off_chip(values), held(two), owner_row, sub_row)

    def exchange(message):
        arrived = lax.all_to_all(message.reshape(peers, MSG, LANES), "shuf", 0, 0, tiled=True)
        return held(arrived.reshape(peers * MSG, LANES))

    arrived = exchange(outgoing)

    slabs = {0: own_slab}
    for d in (1, 3):
        slabs[d] = hop(own_slab, "rep", d)
    for d, sent in ((1, one), (3, three)):
        moved[d] = hop(sent, "rep", d)

    both = pl.pallas_call(
        pair_kernel,
        out_shape=jax.ShapeDtypeStruct((2, cols), F32),
        compiler_params=limit(1),
        name="pair",
    )(col_gain.reshape(1, cols), col_bias.reshape(1, cols))
    answer = pl.pallas_call(
        lambda *refs: owner_kernel(*refs, peers=peers, tile_rows=tile_rows),
        in_specs=[IN_VMEM, whole(2, cols)],
        out_shape=pltpu.HBM((peers * MSG, LANES), BF16),
        scratch_shapes=[pltpu.VMEM((peers * MSG, LANES), F32)],
        compiler_params=limit(6),
        name="moments",
    )(arrived, both)
    returned = exchange(answer)

    def trade(value, distance):
        return lax.ppermute(value, "shuf", [(i, i ^ distance) for i in range(peers)])

    mine = pl.pallas_call(
        stack_kernel,
        grid=(1,),
        in_specs=[whole(slab, outputs), whole(slab, outputs), whole(cols, cols), whole(slab, outputs)],
        out_specs=whole(cols, outputs),
        out_shape=pltpu.HBM((cols, outputs), BF16),
        compiler_params=limit(8),
        name="stack",
    )(slabs[0], slabs[1], moved[2], slabs[3])
    across = trade(mine, 2 * depth)
    sibling = trade(mine, 1)
    across_sibling = trade(across, 1)
    weight = pl.pallas_call(
        lambda *refs: assemble_kernel(*refs, blocks=blocks, cols=cols, depth=depth),
        grid=(1,),
        in_specs=[whole(cols, outputs)] + [IN_VMEM] * 3,
        out_specs=IN_VMEM,
        out_shape=pltpu.VMEM((blocks * cols, outputs), BF16),
        compiler_params=limit(8),
        name="assemble",
    )(off_chip(mine), held(sibling), held(across), held(across_sibling))

    each = tiles // blocks
    coeffs = pl.pallas_call(
        lambda *refs: tile_kernel(*refs, tiles=tiles, peers=peers, blocks=blocks),
        in_specs=[IN_VMEM, whole(1, tiles)],
        out_specs=[IN_VMEM] * blocks,
        out_shape=[pltpu.VMEM((each, 3 * cols), BF16)] * blocks,
        scratch_shapes=[pltpu.VMEM((peers * MSG, LANES), F32)],
        compiler_params=limit(4),
        name="pick",
    )(returned, owner_row)
    known = {0: coeffs[0]}
    for d in (2, 1, 3):
        known[d] = hop(coeffs[d], "rep", d)

    block = min(512, own_rows)
    return pl.pallas_call(
        lambda *refs: project_kernel(
            *refs, blocks=blocks, tile_rows=tile_rows, block=block, skipped=(0, two.shape[0] - own_rows, 0)
        ),
        in_specs=[IN_HBM] * blocks + [IN_VMEM] * (blocks + 1),
        out_specs=IN_HBM,
        out_shape=pltpu.HBM((own_rows, outputs), BF16),
        scratch_shapes=[
            pltpu.VMEM((blocks, own_rows, cols), BF16),
            pltpu.VMEM((own_rows, outputs), BF16),
            pltpu.VMEM((blocks, each, 3 * cols), F32),
            pltpu.SemaphoreType.DMA((blocks, 2)),
            pltpu.SemaphoreType.DMA((own_rows // block,)),
        ],
        compiler_params=limit(24),
        name="project",
    )(
        off_chip(values),
        *[off_chip(moved[d]) for d in range(1, blocks)],
        *[held(known[d]) for d in range(blocks)],
        held(weight),
    )


def solution(mesh):
    return jax.shard_map(
        on_device,
        mesh=mesh,
        in_specs=(P("shuf", "rep"), P("shuf"), P("shuf", None), P("rep"), P("rep"), P("rep", None)),
        out_specs=P(("shuf", "rep"), None),
        check_vma=False,
    )
```

```python
import jax
import jax.numpy as jnp
from jax import lax
from jax.experimental import pallas as pl
from jax.experimental.pallas import tpu as pltpu
from jax.sharding import PartitionSpec as P


GRP_DEV = 32
PRIOR = 256.0
LANES = 128
MSG = 16
F32 = jnp.float32
BF16 = jnp.bfloat16
MIB = 1 << 20


def iota(shape, dim):
    return lax.broadcasted_iota(jnp.int32, shape, dim)


def exact_dot(one_hot, rows):
    return jnp.dot(one_hot.astype(BF16), rows.astype(BF16), preferred_element_type=F32)


def as_column(row, size, at):
    picked = jnp.where(at == iota((size, size), 1), jnp.broadcast_to(row, (size, size)), 0.0)
    return jnp.sum(picked, axis=1, keepdims=True)


def places(owner_row):
    size = owner_row.shape[1]
    column = as_column(owner_row, size, iota((size, size), 0))
    same = column == jnp.broadcast_to(owner_row, (size, size))
    earlier = iota((size, size), 0) < iota((size, size), 1)
    return jnp.sum(jnp.where(same & earlier, 1.0, 0.0), axis=0, keepdims=True)


def put(scratch, part, peers, at):
    for n in range(part.shape[1] // LANES):
        scratch[pl.ds(at + n, peers, stride=MSG), :] = part[:, n * LANES : (n + 1) * LANES]


def take(scratch, peers, at, count):
    return jnp.concatenate([scratch[pl.ds(at + n, peers, stride=MSG), :] for n in range(count)], axis=1)


def run(copies):
    for copy in copies:
        copy.start()
    for copy in copies:
        copy.wait()


def slab_of(depth, slabs):
    index = lax.axis_index("shuf")
    return lax.rem(index // (2 * depth), slabs // 2) * 2 + lax.rem(index, 2)


def cut_kernel(values, weight, out, out_slab, sems, *, rows, blocks, depth):
    slab, cols = out_slab.shape[0], values.shape[1]
    first = pl.multiple_of(lax.rem(lax.axis_index("rep") + 2, blocks) * rows, rows)
    mine = pl.multiple_of(slab_of(depth, weight.shape[0] // slab) * slab, slab)
    copies = [
        pltpu.make_async_copy(values.at[pl.ds(first, rows), :], out.at[pl.ds(blocks * slab, rows), :], sems.at[blocks]),
        pltpu.make_async_copy(weight.at[pl.ds(mine, slab), :], out_slab, sems.at[blocks + 1]),
    ]
    for n in range(blocks):
        source = weight.at[pl.ds(mine, slab), pl.ds(n * cols, cols)]
        copies.append(pltpu.make_async_copy(source, out.at[pl.ds(n * slab, slab), :], sems.at[n]))
    run(copies)


def stack_kernel(own, one, two, three, out):
    slab, cols = own.shape[0], two.shape[1]
    for n, part in ((0, own), (1, one), (3, three)):
        out[n * slab : (n + 1) * slab, :] = part[...]
    for c in range(own.shape[1] // cols):
        out[2 * slab : 3 * slab, c * cols : (c + 1) * cols] = two[c * slab : (c + 1) * slab, :]


def stats_kernel(values, two, owner, sub, out, one, three, *scratches, tiles, peers):
    held_rows, first, second, scratch, sems_in, sems_out = scratches
    rows, cols = one.shape
    blocks, pieces = 4, 2
    here, size = tiles // blocks, rows // pieces
    rank = lax.axis_index("rep")
    tile_rows = rows // here
    chunk = 16
    places_of = {1: held_rows.at[0], 3: held_rows.at[1], 0: held_rows.at[2]}

    def inward(d, p):
        at = pl.multiple_of(lax.rem(rank + d, blocks) * rows + p * size, size)
        target = places_of[d].at[pl.ds(p * size, size), :]
        return pltpu.make_async_copy(values.at[pl.ds(at, size), :], target, sems_in.at[d, p])

    for d in (1, 3, 0):
        for p in range(pieces):
            inward(d, p).start()

    def moments_of(source, d, p):
        def one_tile(t, carry):
            low = high = None
            for n in range(tile_rows // chunk):
                at = pl.multiple_of(t * tile_rows + n * chunk, chunk)
                wide = source[pl.ds(at, chunk), :].astype(F32)
                low, high = (wide, wide * wide) if low is None else (low + wide, high + wide * wide)
            tile = lax.rem(rank + d, blocks) * here + p * (here // pieces) + t
            at = pl.multiple_of(tile * 8, 8)
            for n in range(cols // LANES):
                lanes = slice(n * LANES, (n + 1) * LANES)
                first[n, pl.ds(at, 8), :] = low[:8, lanes] + low[8:, lanes]
                second[n, pl.ds(at, 8), :] = high[:8, lanes] + high[8:, lanes]
            return carry

        lax.fori_loop(0, here // pieces, one_tile, 0, unroll=2)

    skipped = two.shape[0] - rows
    for p in range(pieces):
        moments_of(two.at[pl.ds(skipped + p * size, size), :], 2, p)
    outward = []
    for d in (1, 3, 0):
        for p in range(pieces):
            inward(d, p).wait()
            if d and p == pieces - 1:
                outward.append(pltpu.make_async_copy(places_of[d], one if d == 1 else three, sems_out.at[d // 2]))
                outward[-1].start()
            moments_of(places_of[d].at[pl.ds(p * size, size), :], d, p)

    def folded(ref):
        halves = []
        for n in range(cols // LANES):
            summed = [ref[n, pl.ds(r, tiles, stride=8), :] for r in range(8)]
            while len(summed) > 1:
                summed = [a + b for a, b in zip(summed[::2], summed[1::2])]
            halves.append(summed[0])
        return jnp.concatenate(halves, axis=1) * (1.0 / tile_rows)

    all_mean = folded(first)
    all_var = folded(second) - all_mean * all_mean
    dev_mean = jnp.sum(all_mean, axis=0, keepdims=True) * (1.0 / tiles)
    apart = all_mean - dev_mean
    dev_var = jnp.sum(all_var + apart * apart, axis=0, keepdims=True) * (1.0 / tiles)
    owner_row = owner[...].astype(F32)
    place = places(owner_row)
    named = jnp.broadcast_to(owner_row, (peers, tiles)) == iota((peers, tiles), 0).astype(F32)
    sub_column = as_column(sub[...].astype(F32), tiles, iota((tiles, tiles), 0))
    sub_wide = jnp.broadcast_to(sub_column + 1.0, (tiles, LANES))
    hot = jnp.concatenate([jnp.where(named & (place == float(slot)), 1.0, 0.0) for slot in range(2)], axis=0)
    sent = exact_dot(hot, jnp.concatenate([all_mean, all_var, sub_wide], axis=1))
    for slot in range(2):
        message = sent[slot * peers : (slot + 1) * peers, :]
        put(scratch, message[:, : 2 * cols], peers, 4 * slot)
        put(scratch, message[:, 2 * cols :] - 1.0, peers, 14 + slot)
    high = dev_mean.astype(BF16).astype(F32)
    put(scratch, jnp.broadcast_to(high, (peers, cols)), peers, 8)
    put(scratch, jnp.broadcast_to(dev_mean - high, (peers, cols)), peers, 10)
    put(scratch, jnp.broadcast_to(dev_var, (peers, cols)), peers, 12)
    out[...] = scratch[...].astype(BF16)
    for copy in outward:
        copy.wait()


def pair_kernel(gain, bias, out):
    out[0:1, :] = gain[...]
    out[1:2, :] = bias[...]


def owner_kernel(arrived, both, out, scratch, *, peers, tile_rows):
    scratch[...] = arrived[...].astype(F32)
    dev_mean = take(scratch, peers, 8, 2) + take(scratch, peers, 10, 2)
    mean_all = jnp.sum(dev_mean, axis=0, keepdims=True) * (1.0 / peers)
    apart = dev_mean - mean_all
    var_all = jnp.sum(take(scratch, peers, 12, 2) + apart * apart, axis=0, keepdims=True) * (1.0 / peers)
    cols = dev_mean.shape[1]
    forth, back, firsts, seconds = [], [], [], []
    for slot in range(2):
        label = take(scratch, peers, 14 + slot, 1)
        back.append(jnp.where(label[:, :GRP_DEV] == iota((peers, GRP_DEV), 1).astype(F32), 1.0, 0.0))
        on_diagonal = iota((peers, peers), 0) == iota((peers, peers), 1)
        row = jnp.sum(jnp.where(on_diagonal, label[:, :peers], 0.0), axis=0, keepdims=True)
        wide = jnp.broadcast_to(row, (GRP_DEV, peers))
        forth.append(jnp.where(wide == iota((GRP_DEV, peers), 0).astype(F32), 1.0, 0.0))
        shifted = take(scratch, peers, 4 * slot, 2) - mean_all
        firsts.append(shifted)
        seconds.append(take(scratch, peers, 4 * slot + 2, 2) + shifted * shifted)
    forth = jnp.concatenate(forth, axis=1)
    count = jnp.sum(forth, axis=1, keepdims=True) * float(tile_rows)
    data = jnp.concatenate([jnp.concatenate(firsts, axis=0), jnp.concatenate(seconds, axis=0)], axis=1)
    high = data.astype(BF16).astype(F32)
    middle = (data - high).astype(BF16).astype(F32)
    parts = exact_dot(forth, jnp.concatenate([high, middle, data - high - middle], axis=1))
    sums = (parts[:, : 2 * cols] + parts[:, 2 * cols : 4 * cols] + parts[:, 4 * cols :]) * float(tile_rows)
    portion = 1.0 / (count + PRIOR)
    center = sums[:, :cols] * portion
    second = (sums[:, cols:] + PRIOR * var_all) * portion
    inverse = lax.rsqrt(second - center * center + 1e-05)
    scale = (inverse * both[0:1, :]).astype(BF16).astype(F32)
    shift = both[1:2, :] - (center + mean_all) * scale
    shift_high = shift.astype(BF16).astype(F32)
    reply = exact_dot(
        jnp.concatenate(back, axis=0), jnp.concatenate([scale, shift_high, shift - shift_high], axis=1)
    )
    for slot in range(2):
        put(scratch, reply[slot * peers : (slot + 1) * peers, :], peers, 6 * slot)
    out[...] = scratch[...].astype(BF16)


def tile_kernel(arrived, owner, *refs, tiles, peers, blocks):
    outs, scratch = refs[:-1], refs[-1]
    scratch[...] = arrived[...].astype(F32)
    owner_row = owner[...].astype(F32)
    at = (iota((tiles, tiles), 0) + lax.axis_index("rep") * (tiles // blocks)) % tiles
    place = as_column(places(owner_row), tiles, at)
    named = as_column(owner_row, tiles, at) == iota((tiles, peers), 1).astype(F32)
    hot = jnp.concatenate([jnp.where(named & (place == float(slot)), 1.0, 0.0) for slot in range(2)], axis=1)
    rows = jnp.concatenate([take(scratch, peers, 6 * slot, 6) for slot in range(2)], axis=0)
    picked = exact_dot(hot, rows)
    each = tiles // blocks
    for n, out in enumerate(outs):
        out[...] = picked[n * each : (n + 1) * each, :].astype(BF16)


def project_kernel(*refs, blocks, tile_rows, sizes, skipped, depth):
    moved, coeffs, (mine, *others), out = refs[:blocks], refs[blocks : 2 * blocks], refs[2 * blocks : -7], refs[-7]
    held_rows, weight, result, wide, sems_in, sems_weight = refs[-6:]
    _, rows, cols = held_rows.shape
    skipped = (lax.axis_index("rep") * rows, *skipped)
    parts = ((0, sizes[0]), (sizes[0], rows - sizes[0])) if rows > sizes[0] else ((0, rows),)

    def inward(n, p):
        at, size = parts[p]
        source = moved[n].at[pl.ds(pl.multiple_of(skipped[n] + at, tile_rows), size), :]
        return pltpu.make_async_copy(source, held_rows.at[n, pl.ds(at, size), :], sems_in.at[n, p])

    slab = mine.shape[0] // blocks
    slabs = cols // slab
    own = slab_of(depth, slabs)
    core = lax.rem(own, 2)
    beyond = lax.rem(own + 2, slabs)
    numbers = (own + 1 - 2 * core, beyond, beyond + 1 - 2 * core)

    def rows_of(n, number):
        return weight.at[pl.ds(pl.multiple_of(n * cols + number * slab, slab), slab), :]

    own_slabs = [
        pltpu.make_async_copy(mine.at[pl.ds(n * slab, slab), :], rows_of(n, own), sems_weight.at[n])
        for n in range(blocks)
    ]
    for n in range(blocks):
        inward(n, 0).start()
    for copy in own_slabs:
        copy.start()
    for n in range(blocks):
        if len(parts) > 1:
            inward(n, 1).start()
    for part, number in zip(others, numbers):
        for n in range(blocks):
            rows_of(n, number)[...] = part[n * slab : (n + 1) * slab, :]
    for n in range(blocks):
        wide[n] = coeffs[n][...].astype(F32)
    for copy in own_slabs:
        copy.wait()

    def outward(at, size, j):
        return pltpu.make_async_copy(result.at[pl.ds(at, size), :], out.at[pl.ds(at, size), :], sems_in.at[j % blocks, 2 + j // blocks])

    first, ended = 0, []
    for j, size in enumerate(sizes):
        if j < len(parts):
            for n in range(blocks):
                inward(n, j).wait()
        strips = []
        for t in range(size // tile_rows):
            at = first + t * tile_rows
            scores = []
            for n in range(blocks):
                row = wide[n, at // tile_rows : at // tile_rows + 1, :]
                value = held_rows[n, at : at + tile_rows, :]
                scored = value.astype(F32) * row[:, :cols] + (row[:, cols : 2 * cols] + row[:, 2 * cols :])
                scores.append(scored.astype(BF16))
            strips.append(jnp.concatenate(scores, axis=1))
        product = jnp.dot(jnp.concatenate(strips, axis=0), weight[...], preferred_element_type=F32)
        result[first : first + size, :] = product.astype(BF16)
        ended.append(outward(first, size, j))
        ended[-1].start()
        first += size
    for copy in ended:
        copy.wait()


def hop(value, axis, distance):
    size = lax.axis_size(axis)
    return lax.ppermute(value, axis, [(i, (i + distance) % size) for i in range(size)])


def whole(*shape):
    return pl.BlockSpec(shape, lambda *_: (0,) * len(shape))


IN_VMEM = pl.BlockSpec(memory_space=pltpu.VMEM)
IN_SMEM = pl.BlockSpec(memory_space=pltpu.SMEM)
IN_HBM = pl.BlockSpec(memory_space=pltpu.HBM)


def limit(mib):
    return pltpu.CompilerParams(vmem_limit_bytes=mib * MIB)


def held(value):
    return pltpu.with_memory_space_constraint(value, pltpu.VMEM)


def off_chip(value):
    return pltpu.with_memory_space_constraint(value, pltpu.HBM)


IN_ANY = pl.BlockSpec(memory_space=pl.ANY)


def on_device(values, subgroup, owners, col_gain, col_bias, out_weight):
    rows, cols = values.shape
    tiles = subgroup.shape[0]
    tile_rows = rows // tiles
    peers, blocks = lax.axis_size("shuf"), lax.axis_size("rep")
    own_rows = rows // blocks
    outputs = out_weight.shape[1]
    owner_row, sub_row = owners.reshape(1, tiles), subgroup.reshape(1, tiles)

    depth = max(1, peers // 8)
    slab = cols // 4
    moved = {}
    two, own_slab = pl.pallas_call(
        lambda *refs: cut_kernel(*refs, rows=own_rows, blocks=blocks, depth=depth),
        in_specs=[IN_HBM, IN_HBM],
        out_specs=[IN_VMEM] * 2,
        out_shape=[pltpu.VMEM((cols + own_rows, cols), BF16), pltpu.VMEM((slab, outputs), BF16)],
        scratch_shapes=[pltpu.SemaphoreType.DMA((blocks + 2,))],
        compiler_params=limit(2),
        name="cut",
    )(off_chip(values), off_chip(out_weight))
    moved[2] = hop(two, "rep", 2)

    outgoing, one, three = pl.pallas_call(
        lambda *refs: stats_kernel(*refs, tiles=tiles, peers=peers),
        grid=(1,),
        in_specs=[IN_HBM, IN_VMEM, whole(1, tiles), whole(1, tiles)],
        out_specs=[whole(peers * MSG, LANES), IN_HBM, IN_HBM],
        scratch_shapes=[
            pltpu.VMEM((3, own_rows, cols), BF16),
            pltpu.VMEM((cols // LANES, tiles * 8, LANES), F32),
            pltpu.VMEM((cols // LANES, tiles * 8, LANES), F32),
            pltpu.VMEM((peers * MSG, LANES), F32),
            pltpu.SemaphoreType.DMA((blocks, 2)),
            pltpu.SemaphoreType.DMA((2,)),
        ],
        out_shape=[
            pltpu.HBM((peers * MSG, LANES), BF16), pltpu.HBM((own_rows, cols), BF16), pltpu.HBM((own_rows, cols), BF16)
        ],
        compiler_params=limit(8),
        name="stats",
    )(off_chip(values), held(two), owner_row, sub_row)

    def exchange(message):
        arrived = lax.all_to_all(message.reshape(peers, MSG, LANES), "shuf", 0, 0, tiled=True)
        return held(arrived.reshape(peers * MSG, LANES))

    arrived = exchange(outgoing)

    slabs = {0: own_slab}
    for d in (1, 3):
        slabs[d] = hop(own_slab, "rep", d)
    for d, sent in ((1, one), (3, three)):
        moved[d] = hop(sent, "rep", d)

    both = pl.pallas_call(
        pair_kernel,
        out_shape=jax.ShapeDtypeStruct((2, cols), F32),
        compiler_params=limit(1),
        name="pair",
    )(col_gain.reshape(1, cols), col_bias.reshape(1, cols))
    answer = pl.pallas_call(
        lambda *refs: owner_kernel(*refs, peers=peers, tile_rows=tile_rows),
        in_specs=[IN_VMEM, whole(2, cols)],
        out_shape=pltpu.HBM((peers * MSG, LANES), BF16),
        scratch_shapes=[pltpu.VMEM((peers * MSG, LANES), F32)],
        compiler_params=limit(6),
        name="moments",
    )(arrived, both)
    returned = exchange(answer)

    def trade(value, distance):
        return lax.ppermute(value, "shuf", [(i, i ^ distance) for i in range(peers)])

    mine = pl.pallas_call(
        stack_kernel,
        grid=(1,),
        in_specs=[whole(slab, outputs), whole(slab, outputs), whole(cols, cols), whole(slab, outputs)],
        out_specs=whole(cols, outputs),
        out_shape=pltpu.HBM((cols, outputs), BF16),
        compiler_params=limit(8),
        name="stack",
    )(slabs[0], slabs[1], moved[2], slabs[3])
    across = trade(mine, 2 * depth)
    sibling = trade(mine, 1)
    across_sibling = trade(across, 1)
    each = tiles // blocks
    coeffs = pl.pallas_call(
        lambda *refs: tile_kernel(*refs, tiles=tiles, peers=peers, blocks=blocks),
        in_specs=[IN_VMEM, whole(1, tiles)],
        out_specs=[IN_VMEM] * blocks,
        out_shape=[pltpu.VMEM((each, 3 * cols), BF16)] * blocks,
        scratch_shapes=[pltpu.VMEM((peers * MSG, LANES), F32)],
        compiler_params=limit(4),
        name="pick",
    )(returned, owner_row)
    known = {0: coeffs[0]}
    for d in (2, 1, 3):
        known[d] = hop(coeffs[d], "rep", d)

    middle = own_rows // 4
    sizes = (middle // 2, middle, middle, middle, middle // 2)
    return pl.pallas_call(
        lambda *refs: project_kernel(
            *refs,
            blocks=blocks,
            tile_rows=tile_rows,
            sizes=sizes,
            skipped=(0, two.shape[0] - own_rows, 0),
            depth=depth,
        ),
        in_specs=[IN_HBM] * blocks + [IN_VMEM] * blocks + [IN_HBM] + [IN_VMEM] * 3,
        out_specs=IN_HBM,
        out_shape=pltpu.HBM((own_rows, outputs), BF16),
        scratch_shapes=[
            pltpu.VMEM((blocks, own_rows, cols), BF16),
            pltpu.VMEM((blocks * cols, outputs), BF16),
            pltpu.VMEM((own_rows, outputs), BF16),
            pltpu.VMEM((blocks, each, 3 * cols), F32),
            pltpu.SemaphoreType.DMA((blocks, 4)),
            pltpu.SemaphoreType.DMA((blocks,)),
        ],
        compiler_params=limit(28),
        name="project",
    )(
        off_chip(values),
        *[off_chip(moved[d]) for d in range(1, blocks)],
        *[held(known[d]) for d in range(blocks)],
        off_chip(mine),
        held(sibling),
        held(across),
        held(across_sibling),
    )


def solution(mesh):
    return jax.shard_map(
        on_device,
        mesh=mesh,
        in_specs=(P("shuf", "rep"), P("shuf"), P("shuf", None), P("rep"), P("rep"), P("rep", None)),
        out_specs=P(("shuf", "rep"), None),
        check_vma=False,
    )
```

```python
import jax
import jax.numpy as jnp
from jax import lax
from jax.experimental import pallas as pl
from jax.experimental.pallas import tpu as pltpu
from jax.sharding import PartitionSpec as P


GRP_DEV = 32
PRIOR = 256.0
LANES = 128
MSG = 16
F32 = jnp.float32
BF16 = jnp.bfloat16
MIB = 1 << 20


def iota(shape, dim):
    return lax.broadcasted_iota(jnp.int32, shape, dim)


def exact_dot(one_hot, rows):
    return jnp.dot(one_hot.astype(BF16), rows.astype(BF16), preferred_element_type=F32)


def as_column(row, size, at):
    picked = jnp.where(at == iota((size, size), 1), jnp.broadcast_to(row, (size, size)), 0.0)
    return jnp.sum(picked, axis=1, keepdims=True)


def places(owner_row):
    size = owner_row.shape[1]
    column = as_column(owner_row, size, iota((size, size), 0))
    same = column == jnp.broadcast_to(owner_row, (size, size))
    earlier = iota((size, size), 0) < iota((size, size), 1)
    return jnp.sum(jnp.where(same & earlier, 1.0, 0.0), axis=0, keepdims=True)


def put(scratch, part, peers, at):
    for n in range(part.shape[1] // LANES):
        scratch[pl.ds(at + n, peers, stride=MSG), :] = part[:, n * LANES : (n + 1) * LANES]


def take(scratch, peers, at, count):
    return jnp.concatenate([scratch[pl.ds(at + n, peers, stride=MSG), :] for n in range(count)], axis=1)


def run(copies):
    for copy in copies:
        copy.start()
    for copy in copies:
        copy.wait()


def slabs_of(depth):
    index = lax.axis_index("shuf")
    by_y, by_z = lax.rem(index // (2 * depth), 2), 2 + lax.rem(index // 2, 2)
    first_core = lax.rem(index, 2) == 0
    return jnp.where(first_core, by_y, by_z), jnp.where(first_core, by_z, by_y)


def cut_kernel(values, weight, out, out_slab, sems, *, rows, blocks, depth):
    slab, cols = out_slab.shape[0], values.shape[1]
    first = pl.multiple_of(lax.rem(lax.axis_index("rep") + 2, blocks) * rows, rows)
    mine = pl.multiple_of(slabs_of(depth)[0] * slab, slab)
    copies = [
        pltpu.make_async_copy(values.at[pl.ds(first, rows), :], out.at[pl.ds(blocks * slab, rows), :], sems.at[blocks]),
        pltpu.make_async_copy(weight.at[pl.ds(mine, slab), :], out_slab, sems.at[blocks + 1]),
    ]
    for n in range(blocks):
        source = weight.at[pl.ds(mine, slab), pl.ds(n * cols, cols)]
        copies.append(pltpu.make_async_copy(source, out.at[pl.ds(n * slab, slab), :], sems.at[n]))
    run(copies)


def stack_kernel(own, one, two, three, out):
    slab, cols = own.shape[0], two.shape[1]
    for n, part in ((0, own), (1, one), (3, three)):
        out[n * slab : (n + 1) * slab, :] = part[...]
    for c in range(own.shape[1] // cols):
        out[2 * slab : 3 * slab, c * cols : (c + 1) * cols] = two[c * slab : (c + 1) * slab, :]


def stats_kernel(values, two, owner, sub, out, one, three, *scratches, tiles, peers):
    held_rows, first, second, scratch, sems_in, sems_out = scratches
    rows, cols = one.shape
    blocks, pieces = 4, 2
    here, size = tiles // blocks, rows // pieces
    rank = lax.axis_index("rep")
    tile_rows = rows // here
    chunk = 16
    places_of = {1: held_rows.at[0], 3: held_rows.at[1], 0: held_rows.at[2]}

    def inward(d, p):
        at = pl.multiple_of(lax.rem(rank + d, blocks) * rows + p * size, size)
        target = places_of[d].at[pl.ds(p * size, size), :]
        return pltpu.make_async_copy(values.at[pl.ds(at, size), :], target, sems_in.at[d, p])

    for d in (1, 3, 0):
        for p in range(pieces):
            inward(d, p).start()

    def moments_of(source, d, p):
        def one_tile(t, carry):
            low = high = None
            for n in range(tile_rows // chunk):
                at = pl.multiple_of(t * tile_rows + n * chunk, chunk)
                wide = source[pl.ds(at, chunk), :].astype(F32)
                low, high = (wide, wide * wide) if low is None else (low + wide, high + wide * wide)
            tile = lax.rem(rank + d, blocks) * here + p * (here // pieces) + t
            at = pl.multiple_of(tile * 8, 8)
            for n in range(cols // LANES):
                lanes = slice(n * LANES, (n + 1) * LANES)
                first[n, pl.ds(at, 8), :] = low[:8, lanes] + low[8:, lanes]
                second[n, pl.ds(at, 8), :] = high[:8, lanes] + high[8:, lanes]
            return carry

        lax.fori_loop(0, here // pieces, one_tile, 0, unroll=2)

    skipped = two.shape[0] - rows
    for p in range(pieces):
        moments_of(two.at[pl.ds(skipped + p * size, size), :], 2, p)
    outward = []
    for d in (1, 3, 0):
        for p in range(pieces):
            inward(d, p).wait()
            if d and p == pieces - 1:
                outward.append(pltpu.make_async_copy(places_of[d], one if d == 1 else three, sems_out.at[d // 2]))
                outward[-1].start()
            moments_of(places_of[d].at[pl.ds(p * size, size), :], d, p)

    def folded(ref):
        halves = []
        for n in range(cols // LANES):
            summed = [ref[n, pl.ds(r, tiles, stride=8), :] for r in range(8)]
            while len(summed) > 1:
                summed = [a + b for a, b in zip(summed[::2], summed[1::2])]
            halves.append(summed[0])
        return jnp.concatenate(halves, axis=1) * (1.0 / tile_rows)

    all_mean = folded(first)
    all_var = folded(second) - all_mean * all_mean
    dev_mean = jnp.sum(all_mean, axis=0, keepdims=True) * (1.0 / tiles)
    apart = all_mean - dev_mean
    dev_var = jnp.sum(all_var + apart * apart, axis=0, keepdims=True) * (1.0 / tiles)
    owner_row = owner[...].astype(F32)
    place = places(owner_row)
    named = jnp.broadcast_to(owner_row, (peers, tiles)) == iota((peers, tiles), 0).astype(F32)
    sub_column = as_column(sub[...].astype(F32), tiles, iota((tiles, tiles), 0))
    sub_wide = jnp.broadcast_to(sub_column + 1.0, (tiles, LANES))
    hot = jnp.concatenate([jnp.where(named & (place == float(slot)), 1.0, 0.0) for slot in range(2)], axis=0)
    sent = exact_dot(hot, jnp.concatenate([all_mean, all_var, sub_wide], axis=1))
    for slot in range(2):
        message = sent[slot * peers : (slot + 1) * peers, :]
        put(scratch, message[:, : 2 * cols], peers, 4 * slot)
        put(scratch, message[:, 2 * cols :] - 1.0, peers, 14 + slot)
    high = dev_mean.astype(BF16).astype(F32)
    put(scratch, jnp.broadcast_to(high, (peers, cols)), peers, 8)
    put(scratch, jnp.broadcast_to(dev_mean - high, (peers, cols)), peers, 10)
    put(scratch, jnp.broadcast_to(dev_var, (peers, cols)), peers, 12)
    out[...] = scratch[...].astype(BF16)
    for copy in outward:
        copy.wait()


def pair_kernel(gain, bias, out):
    out[0:1, :] = gain[...]
    out[1:2, :] = bias[...]


def owner_kernel(arrived, both, out, scratch, *, peers, tile_rows):
    scratch[...] = arrived[...].astype(F32)
    dev_mean = take(scratch, peers, 8, 2) + take(scratch, peers, 10, 2)
    mean_all = jnp.sum(dev_mean, axis=0, keepdims=True) * (1.0 / peers)
    apart = dev_mean - mean_all
    var_all = jnp.sum(take(scratch, peers, 12, 2) + apart * apart, axis=0, keepdims=True) * (1.0 / peers)
    cols = dev_mean.shape[1]
    forth, back, firsts, seconds = [], [], [], []
    for slot in range(2):
        label = take(scratch, peers, 14 + slot, 1)
        back.append(jnp.where(label[:, :GRP_DEV] == iota((peers, GRP_DEV), 1).astype(F32), 1.0, 0.0))
        on_diagonal = iota((peers, peers), 0) == iota((peers, peers), 1)
        row = jnp.sum(jnp.where(on_diagonal, label[:, :peers], 0.0), axis=0, keepdims=True)
        wide = jnp.broadcast_to(row, (GRP_DEV, peers))
        forth.append(jnp.where(wide == iota((GRP_DEV, peers), 0).astype(F32), 1.0, 0.0))
        shifted = take(scratch, peers, 4 * slot, 2) - mean_all
        firsts.append(shifted)
        seconds.append(take(scratch, peers, 4 * slot + 2, 2) + shifted * shifted)
    forth = jnp.concatenate(forth, axis=1)
    count = jnp.sum(forth, axis=1, keepdims=True) * float(tile_rows)
    data = jnp.concatenate([jnp.concatenate(firsts, axis=0), jnp.concatenate(seconds, axis=0)], axis=1)
    high = data.astype(BF16).astype(F32)
    middle = (data - high).astype(BF16).astype(F32)
    parts = exact_dot(forth, jnp.concatenate([high, middle, data - high - middle], axis=1))
    sums = (parts[:, : 2 * cols] + parts[:, 2 * cols : 4 * cols] + parts[:, 4 * cols :]) * float(tile_rows)
    portion = 1.0 / (count + PRIOR)
    center = sums[:, :cols] * portion
    second = (sums[:, cols:] + PRIOR * var_all) * portion
    inverse = lax.rsqrt(second - center * center + 1e-05)
    scale = (inverse * both[0:1, :]).astype(BF16).astype(F32)
    shift = both[1:2, :] - (center + mean_all) * scale
    shift_high = shift.astype(BF16).astype(F32)
    reply = exact_dot(
        jnp.concatenate(back, axis=0), jnp.concatenate([scale, shift_high, shift - shift_high], axis=1)
    )
    for slot in range(2):
        put(scratch, reply[slot * peers : (slot + 1) * peers, :], peers, 6 * slot)
    out[...] = scratch[...].astype(BF16)


def tile_kernel(arrived, owner, *refs, tiles, peers, blocks):
    outs, scratch = refs[:-1], refs[-1]
    scratch[...] = arrived[...].astype(F32)
    owner_row = owner[...].astype(F32)
    at = (iota((tiles, tiles), 0) + lax.axis_index("rep") * (tiles // blocks)) % tiles
    place = as_column(places(owner_row), tiles, at)
    named = as_column(owner_row, tiles, at) == iota((tiles, peers), 1).astype(F32)
    hot = jnp.concatenate([jnp.where(named & (place == float(slot)), 1.0, 0.0) for slot in range(2)], axis=1)
    rows = jnp.concatenate([take(scratch, peers, 6 * slot, 6) for slot in range(2)], axis=0)
    picked = exact_dot(hot, rows)
    each = tiles // blocks
    for n, out in enumerate(outs):
        out[...] = picked[n * each : (n + 1) * each, :].astype(BF16)


def project_kernel(*refs, blocks, tile_rows, sizes, skipped, depth):
    moved, coeffs, (mine, *others), out = refs[:blocks], refs[blocks : 2 * blocks], refs[2 * blocks : -7], refs[-7]
    held_rows, weight, result, wide, sems_in, sems_weight = refs[-6:]
    _, rows, cols = held_rows.shape
    skipped = (lax.axis_index("rep") * rows, *skipped)
    parts = ((0, sizes[0]), (sizes[0], rows - sizes[0])) if rows > sizes[0] else ((0, rows),)

    def inward(n, p):
        at, size = parts[p]
        source = moved[n].at[pl.ds(pl.multiple_of(skipped[n] + at, tile_rows), size), :]
        return pltpu.make_async_copy(source, held_rows.at[n, pl.ds(at, size), :], sems_in.at[n, p])

    slab = mine.shape[0] // blocks
    own, beside = slabs_of(depth)
    numbers = (beside, own + 1 - 2 * lax.rem(own, 2), beside + 1 - 2 * lax.rem(beside, 2))

    def rows_of(n, number):
        return weight.at[pl.ds(pl.multiple_of(n * cols + number * slab, slab), slab), :]

    own_slabs = [
        pltpu.make_async_copy(mine.at[pl.ds(n * slab, slab), :], rows_of(n, own), sems_weight.at[n])
        for n in range(blocks)
    ]
    for n in range(blocks):
        inward(n, 0).start()
    for copy in own_slabs:
        copy.start()
    for n in range(blocks):
        if len(parts) > 1:
            inward(n, 1).start()
    for part, number in zip(others, numbers):
        for n in range(blocks):
            rows_of(n, number)[...] = part[n * slab : (n + 1) * slab, :]
    for n in range(blocks):
        wide[n] = coeffs[n][...].astype(F32)
    for copy in own_slabs:
        copy.wait()

    def outward(at, size, j):
        return pltpu.make_async_copy(result.at[pl.ds(at, size), :], out.at[pl.ds(at, size), :], sems_in.at[j % blocks, 2 + j // blocks])

    first, ended = 0, []
    for j, size in enumerate(sizes):
        if j < len(parts):
            for n in range(blocks):
                inward(n, j).wait()
        strips = []
        for t in range(size // tile_rows):
            at = first + t * tile_rows
            scores = []
            for n in range(blocks):
                row = wide[n, at // tile_rows : at // tile_rows + 1, :]
                value = held_rows[n, at : at + tile_rows, :]
                scored = value.astype(F32) * row[:, :cols] + (row[:, cols : 2 * cols] + row[:, 2 * cols :])
                scores.append(scored.astype(BF16))
            strips.append(jnp.concatenate(scores, axis=1))
        product = jnp.dot(jnp.concatenate(strips, axis=0), weight[...], preferred_element_type=F32)
        result[first : first + size, :] = product.astype(BF16)
        ended.append(outward(first, size, j))
        ended[-1].start()
        first += size
    for copy in ended:
        copy.wait()


def hop(value, axis, distance):
    size = lax.axis_size(axis)
    return lax.ppermute(value, axis, [(i, (i + distance) % size) for i in range(size)])


def whole(*shape):
    return pl.BlockSpec(shape, lambda *_: (0,) * len(shape))


IN_VMEM = pl.BlockSpec(memory_space=pltpu.VMEM)
IN_SMEM = pl.BlockSpec(memory_space=pltpu.SMEM)
IN_HBM = pl.BlockSpec(memory_space=pltpu.HBM)


def limit(mib):
    return pltpu.CompilerParams(vmem_limit_bytes=mib * MIB)


def held(value):
    return pltpu.with_memory_space_constraint(value, pltpu.VMEM)


def off_chip(value):
    return pltpu.with_memory_space_constraint(value, pltpu.HBM)


IN_ANY = pl.BlockSpec(memory_space=pl.ANY)


def on_device(values, subgroup, owners, col_gain, col_bias, out_weight):
    rows, cols = values.shape
    tiles = subgroup.shape[0]
    tile_rows = rows // tiles
    peers, blocks = lax.axis_size("shuf"), lax.axis_size("rep")
    own_rows = rows // blocks
    outputs = out_weight.shape[1]
    owner_row, sub_row = owners.reshape(1, tiles), subgroup.reshape(1, tiles)

    depth = max(1, peers // 8)
    slab = cols // 4
    moved = {}
    two, own_slab = pl.pallas_call(
        lambda *refs: cut_kernel(*refs, rows=own_rows, blocks=blocks, depth=depth),
        in_specs=[IN_HBM, IN_HBM],
        out_specs=[IN_VMEM] * 2,
        out_shape=[pltpu.VMEM((cols + own_rows, cols), BF16), pltpu.VMEM((slab, outputs), BF16)],
        scratch_shapes=[pltpu.SemaphoreType.DMA((blocks + 2,))],
        compiler_params=limit(2),
        name="cut",
    )(off_chip(values), off_chip(out_weight))
    moved[2] = hop(two, "rep", 2)

    outgoing, one, three = pl.pallas_call(
        lambda *refs: stats_kernel(*refs, tiles=tiles, peers=peers),
        grid=(1,),
        in_specs=[IN_HBM, IN_VMEM, whole(1, tiles), whole(1, tiles)],
        out_specs=[whole(peers * MSG, LANES), IN_HBM, IN_HBM],
        scratch_shapes=[
            pltpu.VMEM((3, own_rows, cols), BF16),
            pltpu.VMEM((cols // LANES, tiles * 8, LANES), F32),
            pltpu.VMEM((cols // LANES, tiles * 8, LANES), F32),
            pltpu.VMEM((peers * MSG, LANES), F32),
            pltpu.SemaphoreType.DMA((blocks, 2)),
            pltpu.SemaphoreType.DMA((2,)),
        ],
        out_shape=[
            pltpu.HBM((peers * MSG, LANES), BF16), pltpu.HBM((own_rows, cols), BF16), pltpu.HBM((own_rows, cols), BF16)
        ],
        compiler_params=limit(8),
        name="stats",
    )(off_chip(values), held(two), owner_row, sub_row)

    def exchange(message):
        arrived = lax.all_to_all(message.reshape(peers, MSG, LANES), "shuf", 0, 0, tiled=True)
        return held(arrived.reshape(peers * MSG, LANES))

    arrived = exchange(outgoing)

    slabs = {0: own_slab}
    for d in (1, 3):
        slabs[d] = hop(own_slab, "rep", d)
    for d, sent in ((1, one), (3, three)):
        moved[d] = hop(sent, "rep", d)

    both = pl.pallas_call(
        pair_kernel,
        out_shape=jax.ShapeDtypeStruct((2, cols), F32),
        compiler_params=limit(1),
        name="pair",
    )(col_gain.reshape(1, cols), col_bias.reshape(1, cols))
    answer = pl.pallas_call(
        lambda *refs: owner_kernel(*refs, peers=peers, tile_rows=tile_rows),
        in_specs=[IN_VMEM, whole(2, cols)],
        out_shape=pltpu.HBM((peers * MSG, LANES), BF16),
        scratch_shapes=[pltpu.VMEM((peers * MSG, LANES), F32)],
        compiler_params=limit(6),
        name="moments",
    )(arrived, both)
    returned = exchange(answer)

    def trade(value, distance):
        return lax.ppermute(value, "shuf", [(i, i ^ distance) for i in range(peers)])

    mine = pl.pallas_call(
        stack_kernel,
        grid=(1,),
        in_specs=[whole(slab, outputs), whole(slab, outputs), whole(cols, cols), whole(slab, outputs)],
        out_specs=whole(cols, outputs),
        out_shape=pltpu.HBM((cols, outputs), BF16),
        compiler_params=limit(8),
        name="stack",
    )(slabs[0], slabs[1], moved[2], slabs[3])
    pairs = [(i, i ^ (2 if i % 2 else 2 * depth)) for i in range(peers)]
    across = lax.ppermute(mine, "shuf", pairs)
    sibling = trade(mine, 1)
    across_sibling = trade(across, 1)
    each = tiles // blocks
    coeffs = pl.pallas_call(
        lambda *refs: tile_kernel(*refs, tiles=tiles, peers=peers, blocks=blocks),
        in_specs=[IN_VMEM, whole(1, tiles)],
        out_specs=[IN_VMEM] * blocks,
        out_shape=[pltpu.VMEM((each, 3 * cols), BF16)] * blocks,
        scratch_shapes=[pltpu.VMEM((peers * MSG, LANES), F32)],
        compiler_params=limit(4),
        name="pick",
    )(returned, owner_row)
    known = {0: coeffs[0]}
    for d in (2, 1, 3):
        known[d] = hop(coeffs[d], "rep", d)

    middle = own_rows // 4
    sizes = (middle // 2, middle, middle, middle, middle // 2)
    if middle // 2 % tile_rows:
        sizes = (middle,) * 4
    return pl.pallas_call(
        lambda *refs: project_kernel(
            *refs,
            blocks=blocks,
            tile_rows=tile_rows,
            sizes=sizes,
            skipped=(0, two.shape[0] - own_rows, 0),
            depth=depth,
        ),
        in_specs=[IN_HBM] * blocks + [IN_VMEM] * blocks + [IN_HBM] + [IN_VMEM] * 3,
        out_specs=IN_HBM,
        out_shape=pltpu.HBM((own_rows, outputs), BF16),
        scratch_shapes=[
            pltpu.VMEM((blocks, own_rows, cols), BF16),
            pltpu.VMEM((blocks * cols, outputs), BF16),
            pltpu.VMEM((own_rows, outputs), BF16),
            pltpu.VMEM((blocks, each, 3 * cols), F32),
            pltpu.SemaphoreType.DMA((blocks, 4)),
            pltpu.SemaphoreType.DMA((blocks,)),
        ],
        compiler_params=limit(28),
        name="project",
    )(
        off_chip(values),
        *[off_chip(moved[d]) for d in range(1, blocks)],
        *[held(known[d]) for d in range(blocks)],
        off_chip(mine),
        held(sibling),
        held(across),
        held(across_sibling),
    )


def solution(mesh):
    return jax.shard_map(
        on_device,
        mesh=mesh,
        in_specs=(P("shuf", "rep"), P("shuf"), P("shuf", None), P("rep"), P("rep"), P("rep", None)),
        out_specs=P(("shuf", "rep"), None),
        check_vma=False,
    )
```
